256 devices in a mesh: emb: 8 (over z), col: 4 (over y), row: 8 (over x, core).
Axes of the slice: x: 4, y: 4, z: 8, core: 2. Of those that a mesh axis runs over, the one named last changes fastest.
Arguments:
- inter_mask: int32 [2048, 65536], P('row', 'col')
- emb_user: bfloat16 [2048, 128], P(('row', 'col'), 'emb')
- emb_item: bfloat16 [65536, 128], P(('col', 'row'), 'emb')
- triples: int32 [4096, 3], replicated
Outputs:
- output 1: bfloat16 [2048, 128], P(('row', 'col'), 'emb')
- output 2: bfloat16 [65536, 128], P(('col', 'row'), 'emb')
- output 3: float32 [4096], replicated
All inputs are finite; a program needn't handle non-finite values.
Results may differ from the reference program's by a relative error of at most 0.0126005.
Values are sent between devices in bfloat16 or wider.
A program may use at most 768 MiB of HBM per device.

```python
import jax
import jax.numpy as jnp
from jax import lax

NUM_USERS = 2048
NUM_ITEMS = 65536
EMB_DIM = 128
NUM_TRIPLES = 4096
NUM_LAYERS = 3
SPARSITY = 8
NUM_GROUPS = 32


def setup_inputs(seed: int = 0) -> dict:
    key = jax.random.key(seed)
    key_list = jax.random.split(key, 10)
    inter_mask = (jax.random.randint(key_list[0], (NUM_USERS, NUM_ITEMS), 0, SPARSITY) == 0).astype(jnp.int32)
    mean_user = jax.random.normal(key_list[1], (EMB_DIM,), jnp.float32)
    mean_item = jax.random.normal(key_list[2], (EMB_DIM,), jnp.float32)
    noise_user = jax.random.normal(key_list[3], (NUM_USERS, EMB_DIM), jnp.float32)
    noise_item = jax.random.normal(key_list[4], (NUM_ITEMS, EMB_DIM), jnp.float32)
    group_user = jax.random.normal(key_list[8], (NUM_GROUPS, EMB_DIM), jnp.float32)
    group_item = jax.random.normal(key_list[9], (NUM_GROUPS, EMB_DIM), jnp.float32)
    user_group = (jnp.arange(NUM_USERS) * NUM_GROUPS) // NUM_USERS
    item_group = (jnp.arange(NUM_ITEMS) * NUM_GROUPS) // NUM_ITEMS
    emb_user = (0.5 * (mean_user[None, :] + 1.5 * group_user[user_group] + noise_user)).astype(jnp.bfloat16)
    emb_item = (0.5 * (mean_item[None, :] + 1.5 * group_item[item_group] + noise_item)).astype(jnp.bfloat16)
    users = jax.random.randint(key_list[5], (NUM_TRIPLES,), 0, NUM_USERS).at[0].set(NUM_USERS - 1)
    pos_items = jax.random.randint(key_list[6], (NUM_TRIPLES,), 0, NUM_ITEMS).at[0].set(NUM_ITEMS - 1)
    neg_items = jax.random.randint(key_list[7], (NUM_TRIPLES,), 0, NUM_ITEMS).at[1].set(0)
    triples = jnp.stack([users, pos_items, neg_items], axis=1).astype(jnp.int32)
    return {"inter_mask": inter_mask, "emb_user": emb_user, "emb_item": emb_item, "triples": triples}


def reference(inter_mask, emb_user, emb_item, triples):
    deg_user = jnp.maximum(jnp.sum(inter_mask, axis=1), 1).astype(jnp.float32)
    deg_item = jnp.maximum(jnp.sum(inter_mask, axis=0), 1).astype(jnp.float32)
    adj_norm = ((lax.rsqrt(deg_user)[:, None] * inter_mask.astype(jnp.float32)) * lax.rsqrt(deg_item)[None, :]).astype(jnp.bfloat16)

    def layer_step(carry, unused):
        user_cur, item_cur, user_acc, item_acc = carry
        user_next = jnp.dot(adj_norm, item_cur, preferred_element_type=jnp.float32).astype(jnp.bfloat16)
        item_next = jnp.dot(adj_norm.T, user_cur, preferred_element_type=jnp.float32).astype(jnp.bfloat16)
        new_carry = (user_next, item_next, user_acc + user_next.astype(jnp.float32), item_acc + item_next.astype(jnp.float32))
        return new_carry, None

    init_state = (emb_user, emb_item, emb_user.astype(jnp.float32), emb_item.astype(jnp.float32))
    carry_out, scan_ys = lax.scan(layer_step, init_state, None, length=NUM_LAYERS)
    final_user = (carry_out[2] / (NUM_LAYERS + 1)).astype(jnp.bfloat16)
    final_item = (carry_out[3] / (NUM_LAYERS + 1)).astype(jnp.bfloat16)
    e_user = jnp.take(final_user, triples[:, 0], axis=0).astype(jnp.float32)
    e_pos = jnp.take(final_item, triples[:, 1], axis=0).astype(jnp.float32)
    e_neg = jnp.take(final_item, triples[:, 2], axis=0).astype(jnp.float32)
    score = jnp.sum(e_user * (e_pos - e_neg), axis=1)
    bpr_loss = jax.nn.softplus(-score)
    return final_user, final_item, bpr_loss
```

```python
import functools

import jax
import jax.numpy as jnp
from jax import lax
from jax.experimental import pallas as pl
from jax.experimental.pallas import tpu as pltpu
from jax.sharding import PartitionSpec as P

MESH = pl.DeviceIdType.MESH
F32, BF16, I32 = jnp.float32, jnp.bfloat16, jnp.int32
NUM_LAYERS = 3
CHUNK = 512


def each(lo, hi, body):
    def step(i, carry):
        body(i)
        return carry

    lax.fori_loop(lo, hi, step, 0)


def aligned(start, size, unit):
    return pl.ds(pl.multiple_of(start, unit), size)


def lane_dot(lhs, rhs):
    return lax.dot_general(lhs, rhs, (((1,), (1,)), ((), ())), preferred_element_type=F32)


def kernel(dims, mask_hbm, user_in, item_in, trip, out_user, out_item, score_out,
           mask_raw, mask_bf, adj, deg_item, deg_user, user_scale,
           user0_in, user0, item0, item1, item2,
           user1, user2, part_u, recv_u, part_i, recv_i,
           fin_tile, fin_item, item_own, fin_all, part_d, recv_d, zpart, scores,
           sem_raw, sem_one_s, sem_one_r, sem_send,
           sem_item0, sem_user0, sem_di, sem_du, sem_urs, sem_uag, sem_irs, sem_iag,
           sem_own, sem_fin, sem_d, sem_z, sem_sc):
    n_e, n_c, n_r = dims
    n_x, half = n_r // 2, n_e // 2
    n_p = n_c * n_e
    n_b = n_r * n_c
    emb, col, row = lax.axis_index("emb"), lax.axis_index("col"), lax.axis_index("row")
    chip, core = lax.div(row, 2), lax.rem(row, 2)
    rows_u = mask_hbm.shape[0]
    width = item_in.shape[1]
    sub = width // n_e
    cols = item_in.shape[0]
    kd, cu = part_u.shape[1:]
    ni = adj.shape[1]
    piece = ni // n_x
    lanes = cu // n_c
    plane = col * n_e + emb
    block = row * n_c + col
    home = lax.div(emb, half)
    in_half = lax.rem(emb, half)

    def remote(src, dst, send, recv, e, c, r):
        return pltpu.make_async_remote_copy(
            src_ref=src, dst_ref=dst, send_sem=send, recv_sem=recv, device_id=(e, c, r), device_id_type=MESH)

    def raw(i):
        return pltpu.make_async_copy(
            mask_hbm.at[:, aligned(i * width + emb * sub, sub, 128)], mask_raw.at[i], sem_raw.at[i])

    for i in range(n_r):
        raw(i).start()

    here_rows = aligned(in_half * cols, cols, 16)
    here_items = aligned(row * sub, sub, 128)
    mine = home == core

    def item0_copy(q):
        x_to, e_to = lax.div(q, n_e), lax.rem(q, n_e)
        return x_to, e_to, remote(
            item_in.at[:, aligned(e_to * sub, sub, 128)], item0.at[here_rows, here_items],
            sem_send.at[0], sem_item0.at[row * half + in_half], e_to, col, x_to * 2 + home)

    def item0_send(q):
        x_to, e_to, copy = item0_copy(q)

        @pl.when(jnp.logical_not(mine & (x_to == chip) & (e_to == emb)))
        def _():
            copy.start()

    each(0, n_x * n_e, item0_send)

    user_slot = core * n_c + col

    def user0_copy(q):
        c_to, e_to = lax.div(q, n_e), lax.rem(q, n_e)
        return c_to, e_to, remote(
            user_in, user0_in.at[user_slot, here_rows],
            sem_send.at[1], sem_user0.at[user_slot * half + in_half], e_to, c_to, chip * 2 + home)

    def user0_send(q):
        c_to, e_to, copy = user0_copy(q)

        @pl.when(jnp.logical_not(mine & (c_to == col) & (e_to == emb)))
        def _():
            copy.start()

    each(0, n_p, user0_send)

    @pl.when(mine)
    def _():
        item0[here_rows, here_items] = item_in[:, aligned(emb * sub, sub, 128)]
        user0_in[user_slot, here_rows] = user_in[...]

    own_users = aligned(core * rows_u, rows_u, 128)
    for i in range(n_r):
        raw(i).wait()
        mask_bf[own_users, i * sub:(i + 1) * sub] = mask_raw[i].astype(F32).astype(BF16)
    swap = remote(mask_bf.at[own_users], mask_bf.at[own_users], sem_one_s.at[0], sem_one_r.at[0],
                  emb, col, chip * 2 + 1 - core)
    swap.start()
    ones_u = jnp.ones((8, rows_u), BF16)
    deg_item[row] = jnp.dot(ones_u, mask_bf[own_users, :], preferred_element_type=F32)[0:1].astype(I32)

    def di_copy(j):
        r_to = lax.rem(row + j, n_r)
        return remote(deg_item.at[row], deg_item.at[row], sem_send.at[2], sem_di.at[row], emb, col, r_to)

    each(1, n_r, lambda j: di_copy(j).start())
    swap.wait_recv()
    deg_user[plane] = lane_dot(jnp.ones((8, ni), BF16), mask_bf[...])[0:1].astype(I32)

    def around(j):
        q = lax.rem(plane + j, n_p)
        return lax.div(q, n_e), lax.rem(q, n_e)

    def du_copy(j):
        c_to, e_to = around(j)
        return remote(deg_user.at[plane], deg_user.at[plane], sem_send.at[3], sem_du.at[plane], e_to, c_to, row)

    each(1, n_p, lambda j: du_copy(j).start())

    def arrived(buf, sem, slot):
        remote(buf, buf, sem_send.at[0], sem.at[slot], emb, col, row).wait_recv()

    def from_row(j):
        i = lax.rem(row + j, n_r)
        arrived(deg_item.at[i], sem_di, i)

    def from_plane(j):
        i = lax.rem(plane + j, n_p)
        arrived(deg_user.at[i], sem_du, i)

    each(1, n_r, from_row)
    each(1, n_p, from_plane)
    total_i = deg_item[0]
    for i in range(1, n_r):
        total_i = total_i + deg_item[i]
    total_u = deg_user[0]
    for i in range(1, n_p):
        total_u = total_u + deg_user[i]
    inv_item = lax.rsqrt(jnp.maximum(total_i, 1).astype(F32))
    inv_user = lax.rsqrt(jnp.maximum(total_u, 1).astype(F32))
    user_scale[...] = jnp.transpose(jnp.broadcast_to(inv_user, (128, cu)))

    def scale_rows(i):
        rs = aligned(i * 32, 32, 32)
        by_user = user_scale[rs, :]
        for j in range(ni // 128):
            js = slice(j * 128, (j + 1) * 128)
            adj[rs, js] = ((by_user * mask_bf[rs, js].astype(F32)) * inv_item[:, js]).astype(BF16)

    each(0, cu // 32, scale_rows)

    def send_part_u(k):
        def copy(j):
            c_to, e_to = around(j)
            return remote(part_u.at[k, aligned(e_to * 8, 8, 8), aligned(c_to * lanes, lanes, 128)],
                          recv_u.at[k, plane], sem_send.at[4 + k], sem_urs.at[k, plane], e_to, c_to, row)

        each(1, n_p, lambda j: copy(j).start())
        recv_u[k, plane] = part_u[k, aligned(emb * 8, 8, 8), aligned(col * lanes, lanes, 128)]

    def send_part_i(k):
        def copy(j):
            x_to = lax.rem(chip + j, n_x)
            return remote(part_i.at[k, :, aligned(x_to * piece, piece, 128)],
                          recv_i.at[k, chip], sem_send.at[7 + k], sem_irs.at[k, chip], emb, col, x_to * 2 + core)

        each(1, n_x, lambda j: copy(j).start())
        recv_i[k, chip] = part_i[k, :, aligned(chip * piece, piece, 128)]

    def sum_u(k):
        def wait(j):
            i = lax.rem(plane + j, n_p)
            arrived(recv_u.at[k, i], sem_urs.at[k], i)

        each(1, n_p, wait)
        total = recv_u[k, 0]
        for i in range(1, n_p):
            total = total + recv_u[k, i]
        return total.astype(BF16)

    def sum_i(k):
        def wait(j):
            i = lax.rem(chip + j, n_x)
            arrived(recv_i.at[k, i], sem_irs.at[k], i)

        each(1, n_x, wait)
        total = recv_i[k, 0]
        for i in range(1, n_x):
            total = total + recv_i[k, i]
        return total.astype(BF16)

    def share_u(buf, k):
        def copy(j):
            c_to, e_to = around(j)
            return remote(buf.at[plane], buf.at[plane], sem_send.at[10 + k], sem_uag.at[k, plane], e_to, c_to, row)

        each(1, n_p, lambda j: copy(j).start())

    def share_i(buf, k):
        there = aligned(chip * piece, piece, 128)

        def copy(j):
            x_to = lax.rem(chip + j, n_x)
            return remote(buf.at[:, there], buf.at[:, there], sem_send.at[12 + k], sem_iag.at[k, chip],
                          emb, col, x_to * 2 + core)

        each(1, n_x, lambda j: copy(j).start())

    def whole_u(buf, k):
        def wait(j):
            i = lax.rem(plane + j, n_p)
            arrived(buf.at[i], sem_uag.at[k], i)

        each(1, n_p, wait)
        return jnp.concatenate(
            [jnp.concatenate([buf[c * n_e + e].astype(F32) for c in range(n_c)], axis=1) for e in range(n_e)],
            axis=0).astype(BF16)

    def whole_i(buf, k):
        def wait(j):
            i = lax.rem(chip + j, n_x)
            arrived(buf.at[:, aligned(i * piece, piece, 128)], sem_iag.at[k], i)

        each(1, n_x, wait)
        return buf[...]

    def item0_wait(q):
        r_from, e_from = lax.div(q, half), lax.rem(q, half)

        @pl.when(jnp.logical_not(mine & (r_from == row) & (e_from == in_half)))
        def _():
            arrived(item0.at[aligned(e_from * cols, cols, 16), aligned(r_from * sub, sub, 128)], sem_item0, q)

    def user0_wait(q):
        s_from, e_from = lax.div(q, half), lax.rem(q, half)

        @pl.when(jnp.logical_not(mine & (s_from == user_slot) & (e_from == in_half)))
        def _():
            arrived(user0_in.at[s_from, aligned(e_from * cols, cols, 16)], sem_user0, q)

    each(0, n_r * half, item0_wait)
    each(0, 2 * n_c * half, user0_wait)
    user0[...] = jnp.concatenate(
        [user0_in[2 * t].astype(F32) + pltpu.roll(user0_in[2 * t + 1].astype(F32), lanes // 2, 1) for t in range(n_c)],
        axis=1)

    part_u[0] = lane_dot(item0[...], adj[...])
    send_part_u(0)
    part_i[0] = jnp.dot(user0[...].astype(BF16), adj[...], preferred_element_type=F32)
    send_part_i(0)

    own_items = aligned(chip * piece, piece, 128)
    own_rows, own_lanes = aligned(emb * 8, 8, 8), aligned(col * lanes, lanes, 128)
    got = sum_i(0)
    item1[:, own_items] = got
    share_i(item1, 0)
    item_acc = item0[:, own_items].astype(F32) + got.astype(F32)
    got = sum_u(0)
    user1[plane] = got
    share_u(user1, 0)
    user_acc = user0[own_rows, own_lanes] + got.astype(F32)

    part_u[1] = lane_dot(whole_i(item1, 0), adj[...])
    send_part_u(1)
    part_i[1] = jnp.dot(whole_u(user1, 0), adj[...], preferred_element_type=F32)
    send_part_i(1)
    got = sum_i(1)
    item2[:, own_items] = got
    share_i(item2, 1)
    item_acc = item_acc + got.astype(F32)
    got = sum_u(1)
    user2[plane] = got
    share_u(user2, 1)
    user_acc = user_acc + got.astype(F32)

    part_u[2] = lane_dot(whole_i(item2, 1), adj[...])
    send_part_u(2)
    part_i[2] = jnp.dot(whole_u(user2, 1), adj[...], preferred_element_type=F32)
    send_part_i(2)

    item_acc = item_acc + sum_i(2).astype(F32)
    fin_item[...] = (item_acc / (NUM_LAYERS + 1)).astype(BF16)
    back = aligned(emb * sub, sub, 128)

    def own_copy(q):
        e_to, k_to = lax.div(q, 2), lax.rem(q, 2)
        return e_to, k_to, remote(
            fin_item.at[aligned(e_to * cols, cols, 16), aligned(k_to * sub, sub, 128)], item_own.at[:, back],
            sem_send.at[14], sem_own.at[emb], half * core + e_to, col, chip * 2 + k_to)

    def own_send(q):
        e_to, k_to, copy = own_copy(q)

        @pl.when(jnp.logical_not((half * core + e_to == emb) & (k_to == core)))
        def _():
            copy.start()

    each(0, 2 * half, own_send)

    @pl.when(mine)
    def _():
        item_own[:, back] = fin_item[here_rows, aligned(core * sub, sub, 128)]

    user_acc = user_acc + sum_u(2).astype(F32)
    fin_tile[0] = (user_acc / (NUM_LAYERS + 1)).astype(BF16)
    e_fin = half * core + lax.div(emb, 2)
    top, tile = lax.rem(emb, 2), chip * n_c + col
    slot = top * (n_x * n_c) + tile

    def fin_copy(q):
        r_to, c_to = lax.div(q, n_c), lax.rem(q, n_c)
        return r_to, c_to, remote(fin_tile.at[0], fin_all.at[slot], sem_send.at[15], sem_fin.at[slot],
                                  e_fin, c_to, r_to)

    def fin_send(q):
        r_to, c_to, copy = fin_copy(q)

        @pl.when(jnp.logical_not((e_fin == emb) & (r_to == row) & (c_to == col)))
        def _():
            copy.start()

    each(0, n_b, fin_send)

    @pl.when(e_fin == emb)
    def _():
        fin_all[slot] = fin_tile[0]

    def own_wait(e_from):
        @pl.when(jnp.logical_not(mine & (e_from == emb)))
        def _():
            arrived(item_own.at[:, aligned(e_from * sub, sub, 128)], sem_own, e_from)

    each(0, n_e, own_wait)
    out_item[...] = item_own[...]

    n_hi = width // 128
    by_hi = jnp.concatenate([item_own[:, j * 128:(j + 1) * 128] for j in range(n_hi)], axis=0)
    hi_base = (col * n_r + row) * n_hi

    def pick(ids, table, first, count):
        hot = (lax.broadcasted_iota(I32, (128, ids.shape[1]), 0) == (ids & 127)).astype(F32).astype(BF16)
        found = jnp.dot(table, hot, preferred_element_type=F32)
        high = (ids >> 7) - first
        total = jnp.zeros((cols, ids.shape[1]), F32)
        for j in range(count):
            total = total + jnp.where(high == j, found[j * cols:(j + 1) * cols], 0.0)
        return total

    def pick_items(i):
        at = aligned(i * CHUNK, CHUNK, 128)
        part_d[:, at] = pick(trip[1:2, at], by_hi, hi_base, n_hi) - pick(trip[2:3, at], by_hi, hi_base, n_hi)

    each(0, trip.shape[1] // CHUNK, pick_items)

    def d_copy(j):
        q = lax.rem(block + j, n_b)
        return remote(part_d.at[:, aligned(q * 128, 128, 128)], recv_d.at[block], sem_send.at[16], sem_d.at[block],
                      emb, lax.rem(q, n_c), lax.div(q, n_c))

    each(1, n_b, lambda j: d_copy(j).start())
    recv_d[block] = part_d[:, aligned(block * 128, 128, 128)]

    def fin_wait(q):
        k_from = lax.div(emb, half)
        t_from, x_from, c_from = lax.div(q, n_x * n_c), lax.div(lax.rem(q, n_x * n_c), n_c), lax.rem(q, n_c)
        e_from = 2 * lax.rem(emb, half) + t_from

        @pl.when(jnp.logical_not(
            (k_from == core) & (x_from == chip) & (c_from == col) & (e_from == emb)))
        def _():
            arrived(fin_all.at[q], sem_fin, q)

    each(0, 2 * n_x * n_c, fin_wait)
    n_t = n_x * n_c
    here = chip * n_c + lax.div(core * n_c + col, 2)
    wide = jnp.concatenate([fin_all[here], fin_all[n_t + here]], axis=0).astype(F32)
    wide = jnp.where(lax.rem(col, 2) == 1, pltpu.roll(wide, lanes // 2, 1), wide)
    out_user[...] = wide[:, :lanes // 2].astype(BF16)
    by_tile = jnp.concatenate(
        [fin_all[s * n_t + t].astype(F32) for t in range(n_t) for s in range(2)], axis=0).astype(BF16)
    e_user = pick(trip[0:1, aligned(block * 128, 128, 128)], by_tile, 0, n_t)

    def d_wait(j):
        i = lax.rem(block + j, n_b)
        arrived(recv_d.at[i], sem_d, i)

    each(1, n_b, d_wait)
    diff = recv_d[0]
    for i in range(1, n_b):
        diff = diff + recv_d[i]
    zpart[emb] = jnp.sum(e_user * diff, axis=0, keepdims=True)

    def z_copy(j):
        return remote(zpart.at[emb], zpart.at[emb], sem_send.at[17], sem_z.at[emb], lax.rem(emb + j, n_e), col, row)

    def z_wait(j):
        i = lax.rem(emb + j, n_e)
        arrived(zpart.at[i], sem_z, i)

    each(1, n_e, lambda j: z_copy(j).start())
    each(1, n_e, z_wait)
    score = zpart[0]
    for i in range(1, n_e):
        score = score + zpart[i]
    scores[block] = score

    def s_copy(j):
        q = lax.rem(block + j, n_b)
        return remote(scores.at[block], scores.at[block], sem_send.at[18], sem_sc.at[block],
                      emb, lax.rem(q, n_c), lax.div(q, n_c))

    def s_wait(j):
        i = lax.rem(block + j, n_b)
        arrived(scores.at[i], sem_sc, i)

    each(1, n_b, lambda j: s_copy(j).start())
    each(1, n_b, s_wait)
    for i in range(n_b):
        score_out[i:i + 1, :] = scores[i]

    def left(view, i):
        remote(view, view, sem_send.at[i], sem_one_r.at[0], emb, col, row).wait_send()

    swap.wait_send()
    n_mine = jnp.where(mine, 1, 0)
    each(0, n_x * n_e - n_mine, lambda q: left(item_in.at[:, 0:sub], 0))
    each(0, n_p - n_mine, lambda q: left(user_in, 1))
    left(deg_item.at[0:n_r - 1], 2)
    left(deg_user.at[0:n_p - 1], 3)
    for k in range(3):
        left(recv_u.at[k, 0:n_p - 1], 4 + k)
        left(recv_i.at[k, 0:n_x - 1], 7 + k)
    left(user1.at[0:n_p - 1], 10)
    left(user2.at[0:n_p - 1], 11)
    left(item1.at[:, 0:piece * (n_x - 1)], 12)
    left(item2.at[:, 0:piece * (n_x - 1)], 13)
    each(0, 2 * half - n_mine, lambda q: left(item_own.at[:, 0:sub], 14))
    n_fin = n_b - jnp.where(e_fin == emb, 1, 0)
    each(0, n_fin, lambda q: left(fin_tile.at[0], 15))
    left(recv_d.at[0:n_b - 1], 16)
    left(zpart.at[0:n_e - 1], 17)
    left(scores.at[0:n_b - 1], 18)


def solution(mesh):
    dims = n_e, n_c, n_r = mesh.shape["emb"], mesh.shape["col"], mesh.shape["row"]

    def local_fn(mask_blk, user_sh, item_sh, triples):
        rows_u = mask_blk.shape[0]
        width, cols = item_sh.shape
        num_trip = triples.shape[0]
        n_x, n_p, n_b, half = n_r // 2, n_c * n_e, n_r * n_c, n_e // 2
        sub = width // n_e
        ni, cu, kd = n_r * sub, 2 * rows_u, half * cols
        piece, lanes = ni // n_x, cu // n_c
        user_t = jnp.pad(user_sh.T, ((0, 0), (0, lanes - user_sh.shape[0])))
        dma = pltpu.SemaphoreType.DMA
        vmem = pl.BlockSpec(memory_space=pltpu.VMEM)
        scratch = [
            pltpu.VMEM((n_r, rows_u, sub), I32),
            pltpu.VMEM((cu, ni), BF16),
            pltpu.VMEM((cu, ni), BF16),
            pltpu.VMEM((n_r, 1, ni), I32),
            pltpu.VMEM((n_p, 1, cu), I32),
            pltpu.VMEM((cu, 128), F32),
            pltpu.VMEM((2 * n_c, kd, lanes), BF16),
            pltpu.VMEM((kd, cu), F32),
            pltpu.VMEM((kd, ni), BF16),
            pltpu.VMEM((kd, ni), BF16),
            pltpu.VMEM((kd, ni), BF16),
            pltpu.VMEM((n_p, 8, lanes), BF16),
            pltpu.VMEM((n_p, 8, lanes), BF16),
            pltpu.VMEM((3, kd, cu), F32),
            pltpu.VMEM((3, n_p, 8, lanes), F32),
            pltpu.VMEM((3, kd, ni), F32),
            pltpu.VMEM((3, n_x, kd, piece), F32),
            pltpu.VMEM((1, 8, lanes), BF16),
            pltpu.VMEM((kd, piece), BF16),
            pltpu.VMEM((cols, width), BF16),
            pltpu.VMEM((2 * n_x * n_c, 8, lanes), BF16),
            pltpu.VMEM((cols, num_trip), F32),
            pltpu.VMEM((n_b, cols, 128), F32),
            pltpu.VMEM((n_e, 1, 128), F32),
            pltpu.VMEM((n_b, 1, 128), F32),
            dma((n_r,)), dma((1,)), dma((1,)), dma((19,)),
            dma((n_r * half,)), dma((2 * n_c * half,)), dma((n_r,)), dma((n_p,)),
            dma((3, n_p)), dma((2, n_p)), dma((3, n_x)), dma((2, n_x)),
            dma((n_e,)), dma((2 * n_x * n_c,)), dma((n_b,)), dma((n_e,)), dma((n_b,)),
        ]
        user_t, item_t, score = pl.pallas_call(
            functools.partial(kernel, dims),
            out_shape=(jax.ShapeDtypeStruct((cols, user_sh.shape[0]), BF16),
                       jax.ShapeDtypeStruct((cols, width), BF16),
                       jax.ShapeDtypeStruct((n_b, 128), F32)),
            in_specs=[pl.BlockSpec(memory_space=pl.ANY), vmem, vmem, vmem],
            out_specs=(vmem, vmem, vmem),
            scratch_shapes=scratch,
            compiler_params=pltpu.CompilerParams(has_side_effects=True, vmem_limit_bytes=48 << 20),
        )(mask_blk, user_t, item_sh.T, triples.T)
        return user_t.T, item_t.T, jax.nn.softplus(-score.reshape(num_trip))

    return jax.shard_map(
        local_fn, mesh=mesh,
        in_specs=(P("row", "col"), P(("row", "col"), "emb"), P(("col", "row"), "emb"), P()),
        out_specs=(P(("row", "col"), "emb"), P(("col", "row"), "emb"), P()),
        check_vma=False)
```

```python
import functools

import jax
import jax.numpy as jnp
from jax import lax
from jax.experimental import pallas as pl
from jax.experimental.pallas import tpu as pltpu
from jax.sharding import PartitionSpec as P

MESH = pl.DeviceIdType.MESH
F32, BF16, I32 = jnp.float32, jnp.bfloat16, jnp.int32
NUM_LAYERS = 3
CHUNK = 512


def each(lo, hi, body):
    def step(i, carry):
        body(i)
        return carry

    lax.fori_loop(lo, hi, step, 0)


def aligned(start, size, unit):
    return pl.ds(pl.multiple_of(start, unit), size)


def lane_dot(lhs, rhs):
    return lax.dot_general(lhs, rhs, (((1,), (1,)), ((), ())), preferred_element_type=F32)


def kernel(dims, mask_hbm, user_hbm, item_hbm, trip_hbm, out_user, out_item, score_out,
           user_in, user_pack, user_wide, item_in, trip, mask_raw, mask_bf, adj, deg_item, deg_user, user_scale,
           user0_in, user0, item0, item1, item2,
           user1, user2, part_u, recv_u, part_i, recv_i,
           fin_tile, fin_item, item_own, fin_all, part_d, recv_d, zpart, scores,
           sem_raw, sem_in, sem_one_s, sem_one_r, sem_send,
           sem_item0, sem_user0, sem_di, sem_du, sem_urs, sem_uag, sem_irs, sem_iag,
           sem_own, sem_fin, sem_d, sem_z, sem_sc):
    n_e, n_c, n_r = dims
    n_x, half = n_r // 2, n_e // 2
    n_p = n_c * n_e
    n_b = n_r * n_c
    emb, col, row = lax.axis_index("emb"), lax.axis_index("col"), lax.axis_index("row")
    chip, core = lax.div(row, 2), lax.rem(row, 2)
    rows_u = mask_hbm.shape[0]
    width = item_in.shape[1]
    sub = width // n_e
    cols = item_in.shape[0]
    kd, cu = part_u.shape[1:]
    ni = adj.shape[1]
    piece = ni // n_x
    lanes = cu // n_c
    plane = col * n_e + emb
    block = row * n_c + col
    home = lax.div(emb, half)
    in_half = lax.rem(emb, half)

    def remote(src, dst, send, recv, e, c, r):
        return pltpu.make_async_remote_copy(
            src_ref=src, dst_ref=dst, send_sem=send, recv_sem=recv, device_id=(e, c, r), device_id_type=MESH)

    def raw(i):
        return pltpu.make_async_copy(
            mask_hbm.at[:, aligned(i * width + emb * sub, sub, 128)], mask_raw.at[i], sem_raw.at[i])

    fetch = [pltpu.make_async_copy(src, dst, sem_in.at[i]) for i, (src, dst) in enumerate(
        ((user_hbm, user_in), (item_hbm, item_in), (trip_hbm, trip)))]
    for i in range(n_r):
        raw(i).start()
    for copy in fetch:
        copy.start()

    barrier = pltpu.get_barrier_semaphore()

    def hello(e, c, r):
        pl.semaphore_signal(barrier, inc=1, device_id=(e, c, r), device_id_type=MESH)

    def hello_col(j):
        q = lax.rem(row * n_e + emb + j, n_r * n_e)
        hello(lax.rem(q, n_e), col, lax.div(q, n_e))

    def hello_chip(j):
        c_to, left_over = lax.rem(col + 1 + lax.div(j, 2 * n_e), n_c), lax.rem(j, 2 * n_e)
        hello(lax.div(left_over, 2), c_to, chip * 2 + lax.rem(left_over, 2))

    each(1, n_r * n_e, hello_col)
    each(0, 2 * n_e * (n_c - 1), hello_chip)

    own_users = aligned(core * rows_u, rows_u, 128)
    for i in range(n_r):
        raw(i).wait()
        mask_bf[own_users, i * sub:(i + 1) * sub] = mask_raw[i].astype(F32).astype(BF16)
    own_mask = mask_bf[own_users, :]
    deg_item[row] = jnp.dot(jnp.ones((8, rows_u), BF16), own_mask, preferred_element_type=F32)[0:1].astype(I32)
    own_part = core * n_p + plane
    deg_user[own_part] = lane_dot(jnp.ones((8, ni), BF16), own_mask)[0:1].astype(I32)

    fetch[0].wait()
    user_wide[...] = jnp.zeros_like(user_wide)
    user_wide[:, 0:lanes // 2] = user_in[...].astype(F32)
    wide = user_wide[...]
    user_pack[...] = (wide[0:8] + pltpu.roll(wide[8:16], lanes // 2, 1)).astype(BF16)
    fetch[1].wait()
    fetch[2].wait()
    pl.semaphore_wait(barrier, n_r * n_e - 1 + 2 * n_e * (n_c - 1))

    swap = remote(mask_bf.at[own_users], mask_bf.at[own_users], sem_one_s.at[0], sem_one_r.at[0],
                  emb, col, chip * 2 + 1 - core)
    swap.start()

    def di_copy(j):
        r_to = lax.rem(row + j, n_r)
        return remote(deg_item.at[row], deg_item.at[row], sem_send.at[2], sem_di.at[row], emb, col, r_to)

    each(1, n_r, lambda j: di_copy(j).start())

    def around(j):
        q = lax.rem(plane + j, n_p)
        return lax.div(q, n_e), lax.rem(q, n_e)

    def du_copy(j):
        q = lax.rem(own_part + j, 2 * n_p)
        k_to, p_to = lax.div(q, n_p), lax.rem(q, n_p)
        return remote(deg_user.at[own_part], deg_user.at[own_part], sem_send.at[3], sem_du.at[own_part],
                      lax.rem(p_to, n_e), lax.div(p_to, n_e), chip * 2 + k_to)

    each(1, 2 * n_p, lambda j: du_copy(j).start())

    here_rows = aligned(in_half * cols, cols, 16)
    here_items = aligned(row * sub, sub, 128)
    mine = home == core

    user_slot = (core * n_c + col) * half + in_half

    def user0_copy(q):
        c_to, e_to = lax.div(q, n_e), lax.rem(q, n_e)
        return c_to, e_to, remote(user_pack, user0_in.at[user_slot], sem_send.at[1], sem_user0.at[user_slot],
                                  e_to, c_to, chip * 2 + home)

    def user0_send(q):
        c_to, e_to, copy = user0_copy(q)

        @pl.when(jnp.logical_not(mine & (c_to == col) & (e_to == emb)))
        def _():
            copy.start()

    each(0, n_p, user0_send)


    def item0_copy(q):
        x_to, e_to = lax.div(q, n_e), lax.rem(q, n_e)
        return x_to, e_to, remote(
            item_in.at[:, aligned(e_to * sub, sub, 128)], item0.at[here_rows, here_items],
            sem_send.at[0], sem_item0.at[row * half + in_half], e_to, col, x_to * 2 + home)

    def item0_send(q):
        x_to, e_to, copy = item0_copy(q)

        @pl.when(jnp.logical_not(mine & (x_to == chip) & (e_to == emb)))
        def _():
            copy.start()

    each(0, n_x * n_e, item0_send)

    @pl.when(mine)
    def _():
        item0[here_rows, here_items] = item_in[:, aligned(emb * sub, sub, 128)]
        user0_in[user_slot] = user_pack[...]

    def arrived(buf, sem, slot):
        remote(buf, buf, sem_send.at[0], sem.at[slot], emb, col, row).wait_recv()

    def from_row(j):
        i = lax.rem(row + j, n_r)
        arrived(deg_item.at[i], sem_di, i)

    def from_plane(j):
        i = lax.rem(own_part + j, 2 * n_p)
        arrived(deg_user.at[i], sem_du, i)

    each(1, n_r, from_row)
    each(1, 2 * n_p, from_plane)
    total_i = deg_item[0]
    for i in range(1, n_r):
        total_i = total_i + deg_item[i]
    totals = []
    for k in range(2):
        total = deg_user[k * n_p]
        for i in range(1, n_p):
            total = total + deg_user[k * n_p + i]
        totals.append(total)
    total_u = jnp.concatenate(totals, axis=1)
    inv_item = lax.rsqrt(jnp.maximum(total_i, 1).astype(F32))
    inv_user = lax.rsqrt(jnp.maximum(total_u, 1).astype(F32))
    user_scale[...] = jnp.transpose(jnp.broadcast_to(inv_user, (128, cu)))

    def scale_rows(i):
        rs = aligned(i * 32, 32, 32)
        by_user = user_scale[rs, :]
        for j in range(ni // 128):
            js = slice(j * 128, (j + 1) * 128)
            adj[rs, js] = ((by_user * mask_bf[rs, js].astype(F32)) * inv_item[:, js]).astype(BF16)

    swap.wait_recv()
    each(0, cu // 32, scale_rows)

    def send_part_u(k):
        def copy(j):
            c_to, e_to = around(j)
            return remote(part_u.at[k, aligned(e_to * 8, 8, 8), aligned(c_to * lanes, lanes, 128)],
                          recv_u.at[k, plane], sem_send.at[4 + k], sem_urs.at[k, plane], e_to, c_to, row)

        each(1, n_p, lambda j: copy(j).start())
        recv_u[k, plane] = part_u[k, aligned(emb * 8, 8, 8), aligned(col * lanes, lanes, 128)]

    def send_part_i(k):
        def copy(j):
            x_to = lax.rem(chip + j, n_x)
            return remote(part_i.at[k, :, aligned(x_to * piece, piece, 128)],
                          recv_i.at[k, chip], sem_send.at[7 + k], sem_irs.at[k, chip], emb, col, x_to * 2 + core)

        each(1, n_x, lambda j: copy(j).start())
        recv_i[k, chip] = part_i[k, :, aligned(chip * piece, piece, 128)]

    def sum_u(k):
        def wait(j):
            i = lax.rem(plane + j, n_p)
            arrived(recv_u.at[k, i], sem_urs.at[k], i)

        each(1, n_p, wait)
        total = recv_u[k, 0]
        for i in range(1, n_p):
            total = total + recv_u[k, i]
        return total.astype(BF16)

    def sum_i(k):
        def wait(j):
            i = lax.rem(chip + j, n_x)
            arrived(recv_i.at[k, i], sem_irs.at[k], i)

        each(1, n_x, wait)
        total = recv_i[k, 0]
        for i in range(1, n_x):
            total = total + recv_i[k, i]
        return total.astype(BF16)

    def share_u(buf, k):
        def copy(j):
            c_to, e_to = around(j)
            return remote(buf.at[plane], buf.at[plane], sem_send.at[10 + k], sem_uag.at[k, plane], e_to, c_to, row)

        each(1, n_p, lambda j: copy(j).start())

    def share_i(buf, k):
        there = aligned(chip * piece, piece, 128)

        def copy(j):
            x_to = lax.rem(chip + j, n_x)
            return remote(buf.at[:, there], buf.at[:, there], sem_send.at[12 + k], sem_iag.at[k, chip],
                          emb, col, x_to * 2 + core)

        each(1, n_x, lambda j: copy(j).start())

    def whole_u(buf, k):
        def wait(j):
            i = lax.rem(plane + j, n_p)
            arrived(buf.at[i], sem_uag.at[k], i)

        each(1, n_p, wait)
        return jnp.concatenate(
            [jnp.concatenate([buf[c * n_e + e].astype(F32) for c in range(n_c)], axis=1) for e in range(n_e)],
            axis=0).astype(BF16)

    def whole_i(buf, k):
        def wait(j):
            i = lax.rem(chip + j, n_x)
            arrived(buf.at[:, aligned(i * piece, piece, 128)], sem_iag.at[k], i)

        each(1, n_x, wait)
        return buf[...]

    def item0_wait(q):
        r_from, e_from = lax.div(q, half), lax.rem(q, half)

        @pl.when(jnp.logical_not(mine & (r_from == row) & (e_from == in_half)))
        def _():
            arrived(item0.at[aligned(e_from * cols, cols, 16), aligned(r_from * sub, sub, 128)], sem_item0, q)

    def user0_wait(q):
        @pl.when(jnp.logical_not(mine & (q == user_slot)))
        def _():
            arrived(user0_in.at[q], sem_user0, q)

    each(0, 2 * n_c * half, user0_wait)
    low = lax.broadcasted_iota(I32, (8, lanes), 1) < lanes // 2
    for t in range(n_c):
        for i in range(half):
            one = user0_in[2 * t * half + i].astype(F32)
            two = user0_in[(2 * t + 1) * half + i].astype(F32)
            ts = slice(t * lanes, (t + 1) * lanes)
            user0[i * cols:i * cols + 8, ts] = jnp.where(low, one, pltpu.roll(two, lanes // 2, 1))
            user0[i * cols + 8:i * cols + 16, ts] = jnp.where(low, pltpu.roll(one, lanes // 2, 1), two)

    part_i[0] = jnp.dot(user0[...].astype(BF16), adj[...], preferred_element_type=F32)
    send_part_i(0)
    each(0, n_r * half, item0_wait)
    part_u[0] = lane_dot(item0[...], adj[...])
    send_part_u(0)

    own_items = aligned(chip * piece, piece, 128)
    own_rows, own_lanes = aligned(emb * 8, 8, 8), aligned(col * lanes, lanes, 128)
    got = sum_i(0)
    item1[:, own_items] = got
    share_i(item1, 0)
    item_acc = item0[:, own_items].astype(F32) + got.astype(F32)
    got = sum_u(0)
    user1[plane] = got
    share_u(user1, 0)
    user_acc = user0[own_rows, own_lanes] + got.astype(F32)

    part_u[1] = lane_dot(whole_i(item1, 0), adj[...])
    send_part_u(1)
    part_i[1] = jnp.dot(whole_u(user1, 0), adj[...], preferred_element_type=F32)
    send_part_i(1)
    got = sum_u(1)
    user2[plane] = got
    share_u(user2, 1)
    user_acc = user_acc + got.astype(F32)
    got = sum_i(1)
    item2[:, own_items] = got
    share_i(item2, 1)
    item_acc = item_acc + got.astype(F32)

    part_i[2] = jnp.dot(whole_u(user2, 1), adj[...], preferred_element_type=F32)
    send_part_i(2)
    part_u[2] = lane_dot(whole_i(item2, 1), adj[...])
    send_part_u(2)

    item_acc = item_acc + sum_i(2).astype(F32)
    fin_item[...] = (item_acc / (NUM_LAYERS + 1)).astype(BF16)
    back = aligned(emb * sub, sub, 128)

    def own_copy(q):
        e_to, k_to = lax.div(q, 2), lax.rem(q, 2)
        return e_to, k_to, remote(
            fin_item.at[aligned(e_to * cols, cols, 16), aligned(k_to * sub, sub, 128)], item_own.at[:, back],
            sem_send.at[14], sem_own.at[emb], half * core + e_to, col, chip * 2 + k_to)

    def own_send(q):
        e_to, k_to, copy = own_copy(q)

        @pl.when(jnp.logical_not((half * core + e_to == emb) & (k_to == core)))
        def _():
            copy.start()

    each(0, 2 * half, own_send)

    @pl.when(mine)
    def _():
        item_own[:, back] = fin_item[here_rows, aligned(core * sub, sub, 128)]

    user_acc = user_acc + sum_u(2).astype(F32)
    fin_tile[0] = (user_acc / (NUM_LAYERS + 1)).astype(BF16)
    e_fin = half * core + lax.div(emb, 2)
    top, tile = lax.rem(emb, 2), chip * n_c + col
    slot = top * (n_x * n_c) + tile

    def fin_copy(q):
        r_to, c_to = lax.div(q, n_c), lax.rem(q, n_c)
        return r_to, c_to, remote(fin_tile.at[0], fin_all.at[slot], sem_send.at[15], sem_fin.at[slot],
                                  e_fin, c_to, r_to)

    def fin_send(q):
        r_to, c_to, copy = fin_copy(q)

        @pl.when(jnp.logical_not((e_fin == emb) & (r_to == row) & (c_to == col)))
        def _():
            copy.start()

    each(0, n_b, fin_send)

    @pl.when(e_fin == emb)
    def _():
        fin_all[slot] = fin_tile[0]

    def own_wait(e_from):
        @pl.when(jnp.logical_not(mine & (e_from == emb)))
        def _():
            arrived(item_own.at[:, aligned(e_from * sub, sub, 128)], sem_own, e_from)

    each(0, n_e, own_wait)
    out_item[...] = item_own[...]

    n_hi = width // 128
    by_hi = jnp.concatenate([item_own[:, j * 128:(j + 1) * 128] for j in range(n_hi)], axis=0)
    hi_base = (col * n_r + row) * n_hi

    def pick(ids, table, first, count):
        hot = (lax.broadcasted_iota(I32, (128, ids.shape[1]), 0) == (ids & 127)).astype(F32).astype(BF16)
        found = jnp.dot(table, hot, preferred_element_type=F32)
        high = (ids >> 7) - first
        total = jnp.zeros((cols, ids.shape[1]), F32)
        for j in range(count):
            total = total + jnp.where(high == j, found[j * cols:(j + 1) * cols], 0.0)
        return total

    n_chunk, per_chunk = trip.shape[1] // CHUNK, CHUNK // 128

    def d_send(q):
        @pl.when(q != block)
        def _():
            remote(part_d.at[:, aligned(q * 128, 128, 128)], recv_d.at[block], sem_send.at[16], sem_d.at[block],
                   emb, lax.rem(q, n_c), lax.div(q, n_c)).start()

    def pick_items(i):
        chunk = lax.rem(lax.div(block, per_chunk) + i, n_chunk)
        at = aligned(chunk * CHUNK, CHUNK, 128)
        part_d[:, at] = pick(trip[1:2, at], by_hi, hi_base, n_hi) - pick(trip[2:3, at], by_hi, hi_base, n_hi)
        for j in range(per_chunk):
            d_send(chunk * per_chunk + j)

    each(0, n_chunk, pick_items)
    recv_d[block] = part_d[:, aligned(block * 128, 128, 128)]

    def fin_wait(q):
        k_from = lax.div(emb, half)
        t_from, x_from, c_from = lax.div(q, n_x * n_c), lax.div(lax.rem(q, n_x * n_c), n_c), lax.rem(q, n_c)
        e_from = 2 * lax.rem(emb, half) + t_from

        @pl.when(jnp.logical_not(
            (k_from == core) & (x_from == chip) & (c_from == col) & (e_from == emb)))
        def _():
            arrived(fin_all.at[q], sem_fin, q)

    each(0, 2 * n_x * n_c, fin_wait)
    n_t = n_x * n_c
    here = chip * n_c + lax.div(core * n_c + col, 2)
    wide = jnp.concatenate([fin_all[here], fin_all[n_t + here]], axis=0).astype(F32)
    wide = jnp.where(lax.rem(col, 2) == 1, pltpu.roll(wide, lanes // 2, 1), wide)
    out_user[...] = wide[:, :lanes // 2].astype(BF16)
    by_tile = jnp.concatenate(
        [fin_all[s * n_t + t].astype(F32) for t in range(n_t) for s in range(2)], axis=0).astype(BF16)
    e_user = pick(trip[0:1, aligned(block * 128, 128, 128)], by_tile, 0, n_t)

    def d_wait(j):
        i = lax.rem(block + j, n_b)
        arrived(recv_d.at[i], sem_d, i)

    each(1, n_b, d_wait)
    diff = recv_d[0]
    for i in range(1, n_b):
        diff = diff + recv_d[i]
    zpart[emb] = jnp.sum(e_user * diff, axis=0, keepdims=True)

    def z_copy(j):
        return remote(zpart.at[emb], zpart.at[emb], sem_send.at[17], sem_z.at[emb], lax.rem(emb + j, n_e), col, row)

    def z_wait(j):
        i = lax.rem(emb + j, n_e)
        arrived(zpart.at[i], sem_z, i)

    each(1, n_e, lambda j: z_copy(j).start())

    def left(view, i):
        remote(view, view, sem_send.at[i], sem_one_r.at[0], emb, col, row).wait_send()

    swap.wait_send()
    n_mine = jnp.where(mine, 1, 0)
    each(0, n_x * n_e - n_mine, lambda q: left(item_in.at[:, 0:sub], 0))
    each(0, n_p - n_mine, lambda q: left(user_pack, 1))
    left(deg_item.at[0:n_r - 1], 2)
    left(deg_user.at[0:2 * n_p - 1], 3)
    for k in range(3):
        left(recv_u.at[k, 0:n_p - 1], 4 + k)
        left(recv_i.at[k, 0:n_x - 1], 7 + k)
    left(user1.at[0:n_p - 1], 10)
    left(user2.at[0:n_p - 1], 11)
    left(item1.at[:, 0:piece * (n_x - 1)], 12)
    left(item2.at[:, 0:piece * (n_x - 1)], 13)
    each(0, 2 * half - n_mine, lambda q: left(item_own.at[:, 0:sub], 14))
    n_fin = n_b - jnp.where(e_fin == emb, 1, 0)
    each(0, n_fin, lambda q: left(fin_tile.at[0], 15))
    left(recv_d.at[0:n_b - 1], 16)

    each(1, n_e, z_wait)
    score = zpart[0]
    for i in range(1, n_e):
        score = score + zpart[i]
    scores[block] = score

    def s_copy(j):
        q = lax.rem(block + j, n_b)
        return remote(scores.at[block], scores.at[block], sem_send.at[18], sem_sc.at[block],
                      emb, lax.rem(q, n_c), lax.div(q, n_c))

    def s_wait(j):
        i = lax.rem(block + j, n_b)
        arrived(scores.at[i], sem_sc, i)

    each(1, n_b, lambda j: s_copy(j).start())
    each(1, n_b, s_wait)
    for i in range(n_b):
        score_out[i:i + 1, :] = scores[i]
    left(zpart.at[0:n_e - 1], 17)
    left(scores.at[0:n_b - 1], 18)


def solution(mesh):
    dims = n_e, n_c, n_r = mesh.shape["emb"], mesh.shape["col"], mesh.shape["row"]

    def local_fn(mask_blk, user_sh, item_sh, triples):
        rows_u = mask_blk.shape[0]
        width, cols = item_sh.shape
        num_trip = triples.shape[0]
        n_x, n_p, n_b, half = n_r // 2, n_c * n_e, n_r * n_c, n_e // 2
        sub = width // n_e
        ni, cu, kd = n_r * sub, 2 * rows_u, half * cols
        piece, lanes = ni // n_x, cu // n_c
        dma = pltpu.SemaphoreType.DMA
        vmem, hbm = pl.BlockSpec(memory_space=pltpu.VMEM), pl.BlockSpec(memory_space=pl.ANY)
        scratch = [
            pltpu.VMEM((cols, user_sh.shape[0]), BF16),
            pltpu.VMEM((8, lanes), BF16),
            pltpu.VMEM((cols, lanes), F32),
            pltpu.VMEM((cols, width), BF16),
            pltpu.VMEM((3, num_trip), I32),
            pltpu.VMEM((n_r, rows_u, sub), I32),
            pltpu.VMEM((cu, ni), BF16),
            pltpu.VMEM((cu, ni), BF16),
            pltpu.VMEM((n_r, 1, ni), I32),
            pltpu.VMEM((2 * n_p, 1, rows_u), I32),
            pltpu.VMEM((cu, 128), F32),
            pltpu.VMEM((2 * n_c * half, 8, lanes), BF16),
            pltpu.VMEM((kd, cu), F32),
            pltpu.VMEM((kd, ni), BF16),
            pltpu.VMEM((kd, ni), BF16),
            pltpu.VMEM((kd, ni), BF16),
            pltpu.VMEM((n_p, 8, lanes), BF16),
            pltpu.VMEM((n_p, 8, lanes), BF16),
            pltpu.VMEM((3, kd, cu), F32),
            pltpu.VMEM((3, n_p, 8, lanes), F32),
            pltpu.VMEM((3, kd, ni), F32),
            pltpu.VMEM((3, n_x, kd, piece), F32),
            pltpu.VMEM((1, 8, lanes), BF16),
            pltpu.VMEM((kd, piece), BF16),
            pltpu.VMEM((cols, width), BF16),
            pltpu.VMEM((2 * n_x * n_c, 8, lanes), BF16),
            pltpu.VMEM((cols, num_trip), F32),
            pltpu.VMEM((n_b, cols, 128), F32),
            pltpu.VMEM((n_e, 1, 128), F32),
            pltpu.VMEM((n_b, 1, 128), F32),
            dma((n_r,)), dma((3,)), dma((1,)), dma((1,)), dma((19,)),
            dma((n_r * half,)), dma((2 * n_c * half,)), dma((n_r,)), dma((2 * n_p,)),
            dma((3, n_p)), dma((2, n_p)), dma((3, n_x)), dma((2, n_x)),
            dma((n_e,)), dma((2 * n_x * n_c,)), dma((n_b,)), dma((n_e,)), dma((n_b,)),
        ]
        user_t, item_t, score = pl.pallas_call(
            functools.partial(kernel, dims),
            out_shape=(jax.ShapeDtypeStruct((cols, user_sh.shape[0]), BF16),
                       jax.ShapeDtypeStruct((cols, width), BF16),
                       jax.ShapeDtypeStruct((n_b, 128), F32)),
            in_specs=[hbm, hbm, hbm, hbm],
            out_specs=(vmem, vmem, vmem),
            scratch_shapes=scratch,
            compiler_params=pltpu.CompilerParams(collective_id=0, has_side_effects=True, vmem_limit_bytes=48 << 20),
        )(mask_blk, user_sh.T, item_sh.T, triples.T)
        return user_t.T, item_t.T, jax.nn.softplus(-score.reshape(num_trip))

    return jax.shard_map(
        local_fn, mesh=mesh,
        in_specs=(P("row", "col"), P(("row", "col"), "emb"), P(("col", "row"), "emb"), P()),
        out_specs=(P(("row", "col"), "emb"), P(("col", "row"), "emb"), P()),
        check_vma=False)
```

```python
import functools

import jax
import jax.numpy as jnp
from jax import lax
from jax.experimental import pallas as pl
from jax.experimental.pallas import tpu as pltpu
from jax.sharding import PartitionSpec as P

MESH = pl.DeviceIdType.MESH
F32, BF16, I32 = jnp.float32, jnp.bfloat16, jnp.int32
NUM_LAYERS = 3
CHUNK = 512
LOW = 256


def each(lo, hi, body):
    def step(i, carry):
        body(i)
        return carry

    lax.fori_loop(lo, hi, step, 0)


def aligned(start, size, unit):
    return pl.ds(pl.multiple_of(start, unit), size)


def lane_dot(lhs, rhs):
    return lax.dot_general(lhs, rhs, (((1,), (1,)), ((), ())), preferred_element_type=F32)


def far_first(*sizes):
    offsets = [()]
    for n in sizes:
        offsets = [(*o, i) for o in offsets for i in range(n)]
    return sorted(offsets, key=lambda o: -sum(min(i, n - i) for i, n in zip(o, sizes)))


def others(*sizes):
    offsets = [()]
    for n in sizes:
        offsets = [(*o, i) for o in offsets for i in range(n)]
    return offsets[1:]


(S_ITEM0, S_USER0, S_DI, S_DU, S_RU, S_RI, S_GU, S_GI, S_OWN, S_FIN, S_D, S_Z, S_S, S_SWAP, NUM_SEMS) = (
    0, 1, 2, 3, 4, 7, 10, 12, 14, 15, 16, 17, 18, 19, 20)


def kernel(dims, mask_hbm, user_hbm, item_hbm, trip_hbm, out_user, out_item, score_out,
           user_in, user_pack, user_wide, item_in, trip, mask_raw, row_acc, mask_bf, adj, deg_item, deg_user, user_scale,
           user0_in, user0, item0, item1, item2,
           user1, user2, part_u, recv_u, part_i, recv_i,
           fin_tile, fin_item, item_own, fin_all, hot_item, part_d, recv_d, zpart, scores,
           sem_raw, sem_in, sem_send, sem_recv):
    n_e, n_c, n_r = dims
    n_x, half = n_r // 2, n_e // 2
    n_p = n_c * n_e
    n_b = n_r * n_c
    emb, col, row = lax.axis_index("emb"), lax.axis_index("col"), lax.axis_index("row")
    chip, core = lax.div(row, 2), lax.rem(row, 2)
    rows_u = mask_hbm.shape[0]
    width = item_in.shape[1]
    sub = width // n_e
    cols = item_in.shape[0]
    kd, cu = part_u.shape[1:]
    ni = adj.shape[1]
    piece = ni // n_x
    lanes = cu // n_c
    plane = col * n_e + emb
    block = row * n_c + col
    home = lax.div(emb, half)
    in_half = lax.rem(emb, half)
    mine = home == core
    e_at = [lax.rem(emb + i, n_e) for i in range(n_e)]
    c_at = [lax.rem(col + i, n_c) for i in range(n_c)]
    x_at = [lax.rem(chip + i, n_x) for i in range(n_x)]
    k_at = [core, 1 - core]

    def remote(src, dst, stage, e, c, r):
        return pltpu.make_async_remote_copy(
            src_ref=src, dst_ref=dst, send_sem=sem_send.at[stage], recv_sem=sem_recv.at[stage],
            device_id=(e, c, r), device_id_type=MESH)

    def arrived(view, stage):
        remote(view, view, stage, emb, col, row).wait_recv()

    def left(view, stage):
        remote(view, view, stage, emb, col, row).wait_send()

    def either(wait, alone, less, full, stage):
        @pl.when(alone)
        def _():
            wait(less, stage)

        @pl.when(jnp.logical_not(alone))
        def _():
            wait(full, stage)

    def raw(i):
        return pltpu.make_async_copy(
            mask_hbm.at[:, i * width:(i + 1) * width], mask_raw.at[i], sem_raw.at[i])

    fetch = [pltpu.make_async_copy(src, dst, sem_in.at[i]) for i, (src, dst) in enumerate(
        ((user_hbm, user_in), (item_hbm, item_in), (trip_hbm, trip)))]

    barrier = pltpu.get_barrier_semaphore()

    def hello(e, c, r):
        pl.semaphore_signal(barrier, inc=1, device_id=(e, c, r), device_id_type=MESH)

    for x_o, e_o, k_o in far_first(n_x, n_e, 2)[:-1]:
        hello(e_at[e_o], col, x_at[x_o] * 2 + k_at[k_o])
    for c_o, e_o, k_o in far_first(n_c, n_e, 2):
        if c_o:
            hello(e_at[e_o], c_at[c_o], chip * 2 + k_at[k_o])
    for i in range(n_r):
        raw(i).start()
    for copy in fetch:
        copy.start()

    own_users = aligned(core * rows_u, rows_u, 128)
    at_emb = aligned(emb * sub, sub, 128)
    for i in range(n_r):
        raw(i).wait()
        mask_bf[own_users, i * sub:(i + 1) * sub] = mask_raw[i, :, at_emb].astype(F32).astype(BF16)

        def row_sums(t):
            rs = aligned(t * 32, 32, 32)
            total = mask_raw[i, rs, 0:128]
            for j in range(1, width // 128):
                total = total + mask_raw[i, rs, j * 128:(j + 1) * 128]
            row_acc[rs, :] = total if i == 0 else row_acc[rs, :] + total

        each(0, rows_u // 32, row_sums)
    own_mask = mask_bf[own_users, :]
    deg_item[row] = jnp.dot(jnp.ones((8, rows_u), BF16), own_mask, preferred_element_type=F32)[0:1].astype(I32)
    own_part = core * n_c + col
    deg_user[own_part] = jnp.sum(jnp.transpose(row_acc[...].astype(F32)), axis=0, keepdims=True).astype(I32)

    fetch[0].wait()
    user_wide[...] = jnp.zeros_like(user_wide)
    user_wide[:, 0:lanes // 2] = user_in[...].astype(F32)
    wide = user_wide[...]
    user_pack[...] = (wide[0:8] + pltpu.roll(wide[8:16], lanes // 2, 1)).astype(BF16)
    fetch[1].wait()
    fetch[2].wait()
    pl.semaphore_wait(barrier, n_r * n_e - 1 + 2 * n_e * (n_c - 1))

    for c_o, k_o in others(n_c, 2):
        remote(deg_user.at[own_part], deg_user.at[own_part], S_DU, emb, c_at[c_o], chip * 2 + k_at[k_o]).start()
    for x_o, k_o in others(n_x, 2):
        remote(deg_item.at[row], deg_item.at[row], S_DI, emb, col, x_at[x_o] * 2 + k_at[k_o]).start()

    here_rows = aligned(in_half * cols, cols, 16)
    here_items = aligned(row * sub, sub, 128)
    user_slot = (core * n_c + col) * half + in_half

    def user0_send(c_o, e_o):
        remote(user_pack, user0_in.at[user_slot], S_USER0, e_at[e_o], c_at[c_o], chip * 2 + home).start()

    for c_o, e_o in others(n_c, n_e):
        user0_send(c_o, e_o)
    remote(mask_bf.at[own_users], mask_bf.at[own_users], S_SWAP, emb, col, chip * 2 + 1 - core).start()

    def item0_send(x_o, e_o):
        remote(item_in.at[:, aligned(e_at[e_o] * sub, sub, 128)], item0.at[here_rows, here_items], S_ITEM0,
               e_at[e_o], col, x_at[x_o] * 2 + home).start()

    for x_o, e_o in others(n_x, n_e):
        item0_send(x_o, e_o)

    @pl.when(jnp.logical_not(mine))
    def _():
        user0_send(0, 0)
        item0_send(0, 0)

    @pl.when(mine)
    def _():
        item0[here_rows, here_items] = item_in[:, aligned(emb * sub, sub, 128)]
        user0_in[user_slot] = user_pack[...]

    arrived(deg_item.at[0:n_r - 1], S_DI)
    arrived(deg_user.at[0:2 * n_c - 1], S_DU)
    total_i = deg_item[0]
    for i in range(1, n_r):
        total_i = total_i + deg_item[i]
    totals = []
    for k in range(2):
        total = deg_user[k * n_c]
        for i in range(1, n_c):
            total = total + deg_user[k * n_c + i]
        totals.append(total)
    total_u = jnp.concatenate(totals, axis=1)
    inv_item = lax.rsqrt(jnp.maximum(total_i, 1).astype(F32))
    inv_user = lax.rsqrt(jnp.maximum(total_u, 1).astype(F32))
    user_scale[...] = jnp.transpose(jnp.broadcast_to(inv_user, (128, cu)))

    def scale_rows(i):
        rs = aligned(i * 32, 32, 32)
        by_user = user_scale[rs, :]
        for j in range(ni // 128):
            js = slice(j * 128, (j + 1) * 128)
            adj[rs, js] = ((by_user * mask_bf[rs, js].astype(F32)) * inv_item[:, js]).astype(BF16)

    arrived(mask_bf.at[own_users], S_SWAP)
    each(0, cu // 32, scale_rows)

    own_items = aligned(chip * piece, piece, 128)
    own_rows, own_lanes = aligned(emb * 8, 8, 8), aligned(col * lanes, lanes, 128)

    def step_u(k, items):
        pairs = n_c // 2
        mate = lax.rem(col, 2)
        for (p_o,) in far_first(pairs):
            p_to = lax.rem(lax.div(col, 2) + p_o, pairs)
            both = aligned(p_to * 2 * lanes, 2 * lanes, 128)
            part_u[k, :, both] = lane_dot(items, adj[both, :])
            for c_o in (1, 0):
                c_to = p_to * 2 + lax.rem(mate + c_o, 2)
                for (e_o,) in far_first(n_e):
                    tile = part_u.at[k, aligned(e_at[e_o] * 8, 8, 8), aligned(c_to * lanes, lanes, 128)]
                    if p_o or c_o or e_o:
                        remote(tile, recv_u.at[k, plane], S_RU + k, e_at[e_o], c_to, row).start()
                    else:
                        recv_u[k, plane] = tile[...]

    def step_i(k, users):
        for (x_o,) in far_first(n_x):
            there = aligned(x_at[x_o] * piece, piece, 128)
            part = jnp.dot(users, adj[:, there], preferred_element_type=F32)
            if x_o:
                part_i[k, :, there] = part
                remote(part_i.at[k, :, there], recv_i.at[k, chip], S_RI + k, emb, col, x_at[x_o] * 2 + core).start()
            else:
                recv_i[k, chip] = part

    def sum_u(k):
        arrived(recv_u.at[k, 0:n_p - 1], S_RU + k)
        total = recv_u[k, 0]
        for i in range(1, n_p):
            total = total + recv_u[k, i]
        return total.astype(BF16)

    def sum_i(k):
        arrived(recv_i.at[k, 0:n_x - 1], S_RI + k)
        total = recv_i[k, 0]
        for i in range(1, n_x):
            total = total + recv_i[k, i]
        return total.astype(BF16)

    def share_u(buf, k):
        for c_o, e_o in others(n_c, n_e):
            remote(buf.at[plane], buf.at[plane], S_GU + k, e_at[e_o], c_at[c_o], row).start()

    def share_i(buf, k):
        for (x_o,) in others(n_x):
            remote(buf.at[:, own_items], buf.at[:, own_items], S_GI + k, emb, col, x_at[x_o] * 2 + core).start()

    def whole_u(buf, k):
        arrived(buf.at[0:n_p - 1], S_GU + k)
        return jnp.concatenate(
            [jnp.concatenate([buf[c * n_e + e].astype(F32) for c in range(n_c)], axis=1) for e in range(n_e)],
            axis=0).astype(BF16)

    def whole_i(buf, k):
        arrived(buf.at[:, 0:piece * (n_x - 1)], S_GI + k)
        return buf[...]

    either(arrived, mine, user0_in.at[0:n_p - 1], user0_in, S_USER0)
    low = lax.broadcasted_iota(I32, (8, lanes), 1) < lanes // 2
    for t in range(n_c):
        for i in range(half):
            one = user0_in[2 * t * half + i].astype(F32)
            two = user0_in[(2 * t + 1) * half + i].astype(F32)
            ts = slice(t * lanes, (t + 1) * lanes)
            user0[i * cols:i * cols + 8, ts] = jnp.where(low, one, pltpu.roll(two, lanes // 2, 1))
            user0[i * cols + 8:i * cols + 16, ts] = jnp.where(low, pltpu.roll(one, lanes // 2, 1), two)
    step_i(0, user0[...].astype(BF16))
    n_in = n_r * half
    either(arrived, mine, recv_d.at[0:n_in - 1], recv_d.at[0:n_in], S_ITEM0)
    step_u(0, item0[...])

    def one_hot(ids, size):
        return (lax.broadcasted_iota(I32, (size, ids.shape[1]), 0) == lax.rem(ids, size)).astype(F32).astype(BF16)

    def hot_items(i):
        at = aligned(i * CHUNK, CHUNK, 128)
        for j in range(2):
            hot_item[j, :, at] = one_hot(trip[j + 1:j + 2, at], LOW)

    each(0, trip.shape[1] // CHUNK, hot_items)

    got = sum_i(0)
    item1[:, own_items] = got
    share_i(item1, 0)
    item_acc = item0[:, own_items].astype(F32) + got.astype(F32)
    got = sum_u(0)
    user1[plane] = got
    share_u(user1, 0)
    user_acc = user0[own_rows, own_lanes] + got.astype(F32)

    step_u(1, whole_i(item1, 0))
    step_i(1, whole_u(user1, 0))
    got = sum_u(1)
    user2[plane] = got
    share_u(user2, 1)
    user_acc = user_acc + got.astype(F32)
    got = sum_i(1)
    item2[:, own_items] = got
    share_i(item2, 1)
    item_acc = item_acc + got.astype(F32)

    step_i(2, whole_u(user2, 1))
    step_u(2, whole_i(item2, 1))

    item_acc = item_acc + sum_i(2).astype(F32)
    fin_item[...] = (item_acc / (NUM_LAYERS + 1)).astype(BF16)
    back = aligned(emb * sub, sub, 128)

    def own_send(e_o, k_o):
        e_to = lax.rem(in_half + e_o, half)
        remote(fin_item.at[aligned(e_to * cols, cols, 16), aligned(k_at[k_o] * sub, sub, 128)], item_own.at[:, back],
               S_OWN, half * core + e_to, col, chip * 2 + k_at[k_o]).start()

    for e_o, k_o in others(half, 2):
        own_send(e_o, k_o)

    @pl.when(jnp.logical_not(mine))
    def _():
        own_send(0, 0)

    @pl.when(mine)
    def _():
        item_own[:, back] = fin_item[here_rows, aligned(core * sub, sub, 128)]

    user_acc = user_acc + sum_u(2).astype(F32)
    fin_tile[0] = (user_acc / (NUM_LAYERS + 1)).astype(BF16)
    e_fin = half * core + lax.div(emb, 2)
    slot = lax.rem(emb, 2) * (n_x * n_c) + chip * n_c + col
    fin_mine = e_fin == emb

    def fin_send(x_o, c_o, k_o):
        remote(fin_tile.at[0], fin_all.at[slot], S_FIN, e_fin, c_at[c_o], x_at[x_o] * 2 + k_at[k_o]).start()

    for offsets in others(n_x, n_c, 2):
        fin_send(*offsets)

    @pl.when(jnp.logical_not(fin_mine))
    def _():
        fin_send(0, 0, 0)

    @pl.when(fin_mine)
    def _():
        fin_all[slot] = fin_tile[0]

    either(arrived, mine, item_own.at[:, 0:sub * (n_e - 1)], item_own, S_OWN)
    out_item[...] = item_own[...]

    n_hi = width // LOW
    by_hi = jnp.concatenate([item_own[:, j * LOW:(j + 1) * LOW] for j in range(n_hi)], axis=0)
    hi_base = (col * n_r + row) * n_hi

    def pick(hot, high, table, count):
        found = jnp.dot(table, hot, preferred_element_type=F32)
        total = jnp.zeros((cols, high.shape[1]), F32)
        for j in range(count):
            total = total + jnp.where(high == j, found[j * cols:(j + 1) * cols], 0.0)
        return total

    def pick_side(i, at):
        return pick(hot_item[i - 1, :, at], lax.div(trip[i:i + 1, at], LOW) - hi_base, by_hi, n_hi)

    n_chunk, per_chunk = trip.shape[1] // CHUNK, CHUNK // 128

    def d_send(q):
        @pl.when(q != block)
        def _():
            remote(part_d.at[:, aligned(q * 128, 128, 128)], recv_d.at[block], S_D,
                   emb, lax.rem(q, n_c), lax.div(q, n_c)).start()

    def pick_items(i):
        chunk = lax.rem(lax.div(block, per_chunk) + i, n_chunk)
        at = aligned(chunk * CHUNK, CHUNK, 128)
        part_d[:, at] = pick_side(1, at) - pick_side(2, at)
        for j in range(per_chunk):
            d_send(chunk * per_chunk + j)

    each(1, n_chunk + 1, pick_items)
    recv_d[block] = part_d[:, aligned(block * 128, 128, 128)]

    left(mask_bf.at[own_users], S_SWAP)
    either(left, mine, recv_d.at[0:n_in - 1], recv_d.at[0:n_in], S_ITEM0)
    either(left, mine, user0_in.at[0:n_p - 1], user0_in, S_USER0)
    left(deg_item.at[0:n_r - 1], S_DI)
    left(deg_user.at[0:2 * n_c - 1], S_DU)
    for k in range(3):
        left(recv_u.at[k, 0:n_p - 1], S_RU + k)
        left(recv_i.at[k, 0:n_x - 1], S_RI + k)
    left(user1.at[0:n_p - 1], S_GU)
    left(user2.at[0:n_p - 1], S_GU + 1)
    left(item1.at[:, 0:piece * (n_x - 1)], S_GI)
    left(item2.at[:, 0:piece * (n_x - 1)], S_GI + 1)
    either(left, mine, item_own.at[:, 0:sub * (n_e - 1)], item_own, S_OWN)

    either(arrived, fin_mine, fin_all.at[0:n_b - 1], fin_all, S_FIN)
    n_t = n_x * n_c
    here = chip * n_c + lax.div(core * n_c + col, 2)
    wide = jnp.concatenate([fin_all[here], fin_all[n_t + here]], axis=0).astype(F32)
    wide = jnp.where(lax.rem(col, 2) == 1, pltpu.roll(wide, lanes // 2, 1), wide)
    out_user[...] = wide[:, :lanes // 2].astype(BF16)
    by_tile = jnp.concatenate(
        [fin_all[s * n_t + t].astype(F32) for t in range(n_t) for s in range(2)], axis=0).astype(BF16)
    ids = trip[0:1, aligned(block * 128, 128, 128)]
    e_user = pick(one_hot(ids, 128), lax.div(ids, 128), by_tile, n_t)

    arrived(recv_d.at[0:n_b - 1], S_D)
    diff = recv_d[0]
    for i in range(1, n_b):
        diff = diff + recv_d[i]
    zpart[emb] = jnp.sum(e_user * diff, axis=0, keepdims=True)
    for (e_o,) in others(n_e):
        remote(zpart.at[emb], zpart.at[emb], S_Z, e_at[e_o], col, row).start()
    either(left, fin_mine, fin_all.at[0:n_b - 1], fin_all, S_FIN)
    left(recv_d.at[0:n_b - 1], S_D)
    arrived(zpart.at[0:n_e - 1], S_Z)
    score = zpart[0]
    for i in range(1, n_e):
        score = score + zpart[i]
    scores[block] = score
    for x_o, c_o, k_o in others(n_x, n_c, 2):
        remote(scores.at[block], scores.at[block], S_S, emb, c_at[c_o], x_at[x_o] * 2 + k_at[k_o]).start()
    left(zpart.at[0:n_e - 1], S_Z)
    arrived(scores.at[0:n_b - 1], S_S)
    for i in range(n_b):
        score_out[i:i + 1, :] = scores[i]
    left(scores.at[0:n_b - 1], S_S)


def solution(mesh):
    dims = n_e, n_c, n_r = mesh.shape["emb"], mesh.shape["col"], mesh.shape["row"]

    def local_fn(mask_blk, user_sh, item_sh, triples):
        rows_u = mask_blk.shape[0]
        width, cols = item_sh.shape
        num_trip = triples.shape[0]
        n_x, n_p, n_b, half = n_r // 2, n_c * n_e, n_r * n_c, n_e // 2
        sub = width // n_e
        ni, cu, kd = n_r * sub, 2 * rows_u, half * cols
        piece, lanes = ni // n_x, cu // n_c
        dma = pltpu.SemaphoreType.DMA
        vmem, hbm = pl.BlockSpec(memory_space=pltpu.VMEM), pl.BlockSpec(memory_space=pltpu.HBM)
        scratch = [
            pltpu.VMEM((cols, user_sh.shape[0]), BF16),
            pltpu.VMEM((8, lanes), BF16),
            pltpu.VMEM((cols, lanes), F32),
            pltpu.VMEM((cols, width), BF16),
            pltpu.VMEM((3, num_trip), I32),
            pltpu.VMEM((n_r, rows_u, width), I32),
            pltpu.VMEM((rows_u, 128), I32),
            pltpu.VMEM((cu, ni), BF16),
            pltpu.VMEM((cu, ni), BF16),
            pltpu.VMEM((n_r, 1, ni), I32),
            pltpu.VMEM((2 * n_c, 1, rows_u), I32),
            pltpu.VMEM((cu, 128), F32),
            pltpu.VMEM((2 * n_c * half, 8, lanes), BF16),
            pltpu.VMEM((kd, cu), F32),
            pltpu.VMEM((kd, ni), BF16),
            pltpu.VMEM((kd, ni), BF16),
            pltpu.VMEM((kd, ni), BF16),
            pltpu.VMEM((n_p, 8, lanes), BF16),
            pltpu.VMEM((n_p, 8, lanes), BF16),
            pltpu.VMEM((3, kd, cu), F32),
            pltpu.VMEM((3, n_p, 8, lanes), F32),
            pltpu.VMEM((3, kd, ni), F32),
            pltpu.VMEM((3, n_x, kd, piece), F32),
            pltpu.VMEM((1, 8, lanes), BF16),
            pltpu.VMEM((kd, piece), BF16),
            pltpu.VMEM((cols, width), BF16),
            pltpu.VMEM((2 * n_x * n_c, 8, lanes), BF16),
            pltpu.VMEM((2, LOW, num_trip), BF16),
            pltpu.VMEM((cols, num_trip), F32),
            pltpu.VMEM((n_b, cols, 128), F32),
            pltpu.VMEM((n_e, 1, 128), F32),
            pltpu.VMEM((n_b, 1, 128), F32),
            dma((n_r,)), dma((3,)), dma((NUM_SEMS,)), dma((NUM_SEMS,)),
        ]
        user_t, item_t, score = pl.pallas_call(
            functools.partial(kernel, dims),
            out_shape=(jax.ShapeDtypeStruct((cols, user_sh.shape[0]), BF16),
                       jax.ShapeDtypeStruct((cols, width), BF16),
                       jax.ShapeDtypeStruct((n_b, 128), F32)),
            in_specs=[hbm, hbm, hbm, hbm],
            out_specs=(vmem, vmem, vmem),
            scratch_shapes=scratch,
            compiler_params=pltpu.CompilerParams(collective_id=0, has_side_effects=True, vmem_limit_bytes=40 << 20),
        )(mask_blk, *(pltpu.with_memory_space_constraint(v.T, pltpu.HBM) for v in (user_sh, item_sh, triples)))
        return user_t.T, item_t.T, jax.nn.softplus(-score.reshape(num_trip))

    return jax.shard_map(
        local_fn, mesh=mesh,
        in_specs=(P("row", "col"), P(("row", "col"), "emb"), P(("col", "row"), "emb"), P()),
        out_specs=(P(("row", "col"), "emb"), P(("col", "row"), "emb"), P()),
        check_vma=False)
```

```python
import functools

import jax
import jax.numpy as jnp
from jax import lax
from jax.experimental import pallas as pl
from jax.experimental.pallas import tpu as pltpu
from jax.sharding import PartitionSpec as P

MESH = pl.DeviceIdType.MESH
F32, BF16, I32 = jnp.float32, jnp.bfloat16, jnp.int32
NUM_LAYERS = 3
CHUNK = 512
PICK = 1024
LOW = 256


def each(lo, hi, body):
    def step(i, carry):
        body(i)
        return carry

    lax.fori_loop(lo, hi, step, 0)


def aligned(start, size, unit):
    return pl.ds(pl.multiple_of(start, unit), size)


def lane_dot(lhs, rhs):
    return lax.dot_general(lhs, rhs, (((1,), (1,)), ((), ())), preferred_element_type=F32)


def far_first(*sizes):
    offsets = [()]
    for n in sizes:
        offsets = [(*o, i) for o in offsets for i in range(n)]
    return sorted(offsets, key=lambda o: -sum(min(i, n - i) for i, n in zip(o, sizes)))


def others(*sizes):
    offsets = [()]
    for n in sizes:
        offsets = [(*o, i) for o in offsets for i in range(n)]
    return offsets[1:]


(S_ITEM0, S_USER0, S_DI, S_DU, S_RU, S_RI, S_GU, S_GI, S_OWN, S_FIN, S_D, S_Z, S_S, S_SWAP, NUM_SEMS) = (
    0, 1, 2, 3, 4, 7, 10, 12, 14, 15, 16, 17, 18, 19, 20)


def kernel(dims, mask_hbm, user_hbm, item_hbm, trip_hbm, out_user, out_item, score_out,
           user_in, user_pack, user_wide, item_in, trip, mask_part, mask_raw, row_acc, mask_bf, adj, deg_item, deg_user, user_scale,
           user0_in, user0, item0, item1, item2,
           user1, user2, part_u, recv_u, part_i, recv_i,
           fin_tile, fin_item, item_own, fin_all, hot_item, part_d, recv_d, zpart, scores,
           sem_part, sem_raw, sem_in, sem_send, sem_recv):
    n_e, n_c, n_r = dims
    n_x, half = n_r // 2, n_e // 2
    n_p = n_c * n_e
    n_b = n_r * n_c
    emb, col, row = lax.axis_index("emb"), lax.axis_index("col"), lax.axis_index("row")
    chip, core = lax.div(row, 2), lax.rem(row, 2)
    rows_u = mask_hbm.shape[0]
    width = item_in.shape[1]
    sub = width // n_e
    cols = item_in.shape[0]
    kd, cu = part_u.shape[1:]
    ni = adj.shape[1]
    piece = ni // n_x
    lanes = cu // n_c
    plane = col * n_e + emb
    block = row * n_c + col
    home = lax.div(emb, half)
    in_half = lax.rem(emb, half)
    mine = home == core
    e_at = [lax.rem(emb + i, n_e) for i in range(n_e)]
    c_at = [lax.rem(col + i, n_c) for i in range(n_c)]
    x_at = [lax.rem(chip + i, n_x) for i in range(n_x)]
    k_at = [core, 1 - core]

    def remote(src, dst, stage, e, c, r):
        return pltpu.make_async_remote_copy(
            src_ref=src, dst_ref=dst, send_sem=sem_send.at[stage], recv_sem=sem_recv.at[stage],
            device_id=(e, c, r), device_id_type=MESH)

    def arrived(view, stage):
        remote(view, view, stage, emb, col, row).wait_recv()

    def left(view, stage):
        remote(view, view, stage, emb, col, row).wait_send()

    def either(wait, alone, less, full, stage):
        @pl.when(alone)
        def _():
            wait(less, stage)

        @pl.when(jnp.logical_not(alone))
        def _():
            wait(full, stage)

    def part(i):
        return pltpu.make_async_copy(
            mask_hbm.at[:, aligned(i * width + emb * sub, sub, 128)], mask_part.at[i], sem_part.at[i])

    def raw(i):
        return pltpu.make_async_copy(
            mask_hbm.at[:, i * width:(i + 1) * width], mask_raw.at[i], sem_raw.at[i])

    fetch = [pltpu.make_async_copy(src, dst, sem_in.at[i]) for i, (src, dst) in enumerate(
        ((user_hbm, user_in), (item_hbm, item_in), (trip_hbm, trip)))]

    barrier = pltpu.get_barrier_semaphore()

    def hello(e, c, r):
        pl.semaphore_signal(barrier, inc=1, device_id=(e, c, r), device_id_type=MESH)

    for x_o, e_o, k_o in far_first(n_x, n_e, 2)[:-1]:
        hello(e_at[e_o], col, x_at[x_o] * 2 + k_at[k_o])
    for c_o, e_o, k_o in far_first(n_c, n_e, 2):
        if c_o:
            hello(e_at[e_o], c_at[c_o], chip * 2 + k_at[k_o])
    for copy in fetch:
        copy.start()
    for i in range(n_r):
        part(i).start()
    for i in range(n_r):
        raw(i).start()

    own_users = aligned(core * rows_u, rows_u, 128)
    for i in range(n_r):
        part(i).wait()
        mask_bf[own_users, i * sub:(i + 1) * sub] = mask_part[i].astype(F32).astype(BF16)
    deg_item[row] = jnp.dot(
        jnp.ones((8, rows_u), BF16), mask_bf[own_users, :], preferred_element_type=F32)[0:1].astype(I32)

    fetch[0].wait()
    user_wide[...] = jnp.zeros_like(user_wide)
    user_wide[:, 0:lanes // 2] = user_in[...].astype(F32)
    wide = user_wide[...]
    user_pack[...] = (wide[0:8] + pltpu.roll(wide[8:16], lanes // 2, 1)).astype(BF16)
    fetch[1].wait()
    fetch[2].wait()
    pl.semaphore_wait(barrier, n_r * n_e - 1 + 2 * n_e * (n_c - 1))

    for x_o, k_o in others(n_x, 2):
        remote(deg_item.at[row], deg_item.at[row], S_DI, emb, col, x_at[x_o] * 2 + k_at[k_o]).start()

    here_rows = aligned(in_half * cols, cols, 16)
    here_items = aligned(row * sub, sub, 128)
    user_slot = (core * n_c + col) * half + in_half

    def user0_send(c_o, e_o):
        remote(user_pack, user0_in.at[user_slot], S_USER0, e_at[e_o], c_at[c_o], chip * 2 + home).start()

    for c_o, e_o in others(n_c, n_e):
        user0_send(c_o, e_o)
    remote(mask_bf.at[own_users], mask_bf.at[own_users], S_SWAP, emb, col, chip * 2 + 1 - core).start()

    def item0_send(x_o, e_o):
        remote(item_in.at[:, aligned(e_at[e_o] * sub, sub, 128)], item0.at[here_rows, here_items], S_ITEM0,
               e_at[e_o], col, x_at[x_o] * 2 + home).start()

    for x_o, e_o in others(n_x, n_e):
        item0_send(x_o, e_o)

    @pl.when(jnp.logical_not(mine))
    def _():
        user0_send(0, 0)
        item0_send(0, 0)

    @pl.when(mine)
    def _():
        item0[here_rows, here_items] = item_in[:, aligned(emb * sub, sub, 128)]
        user0_in[user_slot] = user_pack[...]

    for i in range(n_r):
        raw(i).wait()

        def row_sums(t):
            rs = aligned(t * 32, 32, 32)
            total = mask_raw[i, rs, 0:128]
            for j in range(1, width // 128):
                total = total + mask_raw[i, rs, j * 128:(j + 1) * 128]
            row_acc[rs, :] = total if i == 0 else row_acc[rs, :] + total

        each(0, rows_u // 32, row_sums)
    own_part = core * n_c + col
    deg_user[own_part] = jnp.sum(jnp.transpose(row_acc[...].astype(F32)), axis=0, keepdims=True).astype(I32)
    for c_o, k_o in others(n_c, 2):
        remote(deg_user.at[own_part], deg_user.at[own_part], S_DU, emb, c_at[c_o], chip * 2 + k_at[k_o]).start()

    def one_hot(ids, size):
        return (lax.broadcasted_iota(I32, (size, ids.shape[1]), 0) == lax.rem(ids, size)).astype(F32).astype(BF16)

    def hot_items(i):
        at = aligned(i * CHUNK, CHUNK, 128)
        for j in range(2):
            hot_item[j, :, at] = one_hot(trip[j + 1:j + 2, at], LOW)

    each(0, trip.shape[1] // CHUNK, hot_items)

    arrived(deg_item.at[0:n_r - 1], S_DI)
    arrived(deg_user.at[0:2 * n_c - 1], S_DU)
    total_i = deg_item[0]
    for i in range(1, n_r):
        total_i = total_i + deg_item[i]
    totals = []
    for k in range(2):
        total = deg_user[k * n_c]
        for i in range(1, n_c):
            total = total + deg_user[k * n_c + i]
        totals.append(total)
    total_u = jnp.concatenate(totals, axis=1)
    inv_item = lax.rsqrt(jnp.maximum(total_i, 1).astype(F32))
    inv_user = lax.rsqrt(jnp.maximum(total_u, 1).astype(F32))
    user_scale[...] = jnp.transpose(jnp.broadcast_to(inv_user, (128, cu)))

    def scale_rows(i):
        rs = aligned(i * 32, 32, 32)
        by_user = user_scale[rs, :]
        for j in range(ni // 128):
            js = slice(j * 128, (j + 1) * 128)
            adj[rs, js] = ((by_user * mask_bf[rs, js].astype(F32)) * inv_item[:, js]).astype(BF16)

    arrived(mask_bf.at[own_users], S_SWAP)
    each(0, cu // 32, scale_rows)

    own_items = aligned(chip * piece, piece, 128)
    own_rows, own_lanes = aligned(emb * 8, 8, 8), aligned(col * lanes, lanes, 128)

    def step_u(k, items):
        pairs = n_c // 2
        mate = lax.rem(col, 2)
        for (p_o,) in far_first(pairs):
            p_to = lax.rem(lax.div(col, 2) + p_o, pairs)
            both = aligned(p_to * 2 * lanes, 2 * lanes, 128)
            part_u[k, :, both] = lane_dot(items, adj[both, :])
            for c_o in (1, 0):
                c_to = p_to * 2 + lax.rem(mate + c_o, 2)
                for (e_o,) in far_first(n_e):
                    tile = part_u.at[k, aligned(e_at[e_o] * 8, 8, 8), aligned(c_to * lanes, lanes, 128)]
                    if p_o or c_o or e_o:
                        remote(tile, recv_u.at[k, plane], S_RU + k, e_at[e_o], c_to, row).start()
                    else:
                        recv_u[k, plane] = tile[...]

    def step_i(k, users):
        for (x_o,) in far_first(n_x):
            there = aligned(x_at[x_o] * piece, piece, 128)
            part = jnp.dot(users, adj[:, there], preferred_element_type=F32)
            if x_o:
                part_i[k, :, there] = part
                remote(part_i.at[k, :, there], recv_i.at[k, chip], S_RI + k, emb, col, x_at[x_o] * 2 + core).start()
            else:
                recv_i[k, chip] = part

    def sum_u(k):
        arrived(recv_u.at[k, 0:n_p - 1], S_RU + k)
        total = recv_u[k, 0]
        for i in range(1, n_p):
            total = total + recv_u[k, i]
        return total.astype(BF16)

    def sum_i(k):
        arrived(recv_i.at[k, 0:n_x - 1], S_RI + k)
        total = recv_i[k, 0]
        for i in range(1, n_x):
            total = total + recv_i[k, i]
        return total.astype(BF16)

    def share_u(buf, k):
        for c_o, e_o in others(n_c, n_e):
            remote(buf.at[plane], buf.at[plane], S_GU + k, e_at[e_o], c_at[c_o], row).start()

    def share_i(buf, k):
        for (x_o,) in others(n_x):
            remote(buf.at[:, own_items], buf.at[:, own_items], S_GI + k, emb, col, x_at[x_o] * 2 + core).start()

    def whole_u(buf, k):
        arrived(buf.at[0:n_p - 1], S_GU + k)
        return jnp.concatenate(
            [jnp.concatenate([buf[c * n_e + e].astype(F32) for c in range(n_c)], axis=1) for e in range(n_e)],
            axis=0).astype(BF16)

    def whole_i(buf, k):
        arrived(buf.at[:, 0:piece * (n_x - 1)], S_GI + k)
        return buf[...]

    either(arrived, mine, user0_in.at[0:n_p - 1], user0_in, S_USER0)
    low = lax.broadcasted_iota(I32, (8, lanes), 1) < lanes // 2
    for t in range(n_c):
        for i in range(half):
            one = user0_in[2 * t * half + i].astype(F32)
            two = user0_in[(2 * t + 1) * half + i].astype(F32)
            ts = slice(t * lanes, (t + 1) * lanes)
            user0[i * cols:i * cols + 8, ts] = jnp.where(low, one, pltpu.roll(two, lanes // 2, 1))
            user0[i * cols + 8:i * cols + 16, ts] = jnp.where(low, pltpu.roll(one, lanes // 2, 1), two)
    step_i(0, user0[...].astype(BF16))
    n_in = n_r * half
    either(arrived, mine, recv_d.at[0:n_in - 1], recv_d.at[0:n_in], S_ITEM0)
    step_u(0, item0[...])

    got = sum_i(0)
    item1[:, own_items] = got
    share_i(item1, 0)
    item_acc = item0[:, own_items].astype(F32) + got.astype(F32)
    got = sum_u(0)
    user1[plane] = got
    share_u(user1, 0)
    user_acc = user0[own_rows, own_lanes] + got.astype(F32)

    step_u(1, whole_i(item1, 0))
    step_i(1, whole_u(user1, 0))
    got = sum_u(1)
    user2[plane] = got
    share_u(user2, 1)
    user_acc = user_acc + got.astype(F32)
    got = sum_i(1)
    item2[:, own_items] = got
    share_i(item2, 1)
    item_acc = item_acc + got.astype(F32)

    step_i(2, whole_u(user2, 1))
    step_u(2, whole_i(item2, 1))

    item_acc = item_acc + sum_i(2).astype(F32)
    fin_item[...] = (item_acc / (NUM_LAYERS + 1)).astype(BF16)
    back = aligned(emb * sub, sub, 128)

    def own_send(e_o, k_o):
        e_to = lax.rem(in_half + e_o, half)
        remote(fin_item.at[aligned(e_to * cols, cols, 16), aligned(k_at[k_o] * sub, sub, 128)], item_own.at[:, back],
               S_OWN, half * core + e_to, col, chip * 2 + k_at[k_o]).start()

    for e_o, k_o in others(half, 2):
        own_send(e_o, k_o)

    @pl.when(jnp.logical_not(mine))
    def _():
        own_send(0, 0)

    @pl.when(mine)
    def _():
        item_own[:, back] = fin_item[here_rows, aligned(core * sub, sub, 128)]

    user_acc = user_acc + sum_u(2).astype(F32)
    fin_tile[0] = (user_acc / (NUM_LAYERS + 1)).astype(BF16)
    e_fin = half * core + lax.div(emb, 2)
    slot = lax.rem(emb, 2) * (n_x * n_c) + chip * n_c + col
    fin_mine = e_fin == emb

    def fin_send(x_o, c_o, k_o):
        remote(fin_tile.at[0], fin_all.at[slot], S_FIN, e_fin, c_at[c_o], x_at[x_o] * 2 + k_at[k_o]).start()

    for offsets in others(n_x, n_c, 2):
        fin_send(*offsets)

    @pl.when(jnp.logical_not(fin_mine))
    def _():
        fin_send(0, 0, 0)

    @pl.when(fin_mine)
    def _():
        fin_all[slot] = fin_tile[0]

    either(arrived, mine, item_own.at[:, 0:sub * (n_e - 1)], item_own, S_OWN)
    out_item[...] = item_own[...]

    n_hi = width // LOW
    by_hi = jnp.concatenate([item_own[:, j * LOW:(j + 1) * LOW] for j in range(n_hi)], axis=0)
    hi_base = (col * n_r + row) * n_hi

    def pick(hot, high, table, count):
        found = jnp.dot(table, hot, preferred_element_type=F32)
        total = jnp.zeros((cols, high.shape[1]), F32)
        for j in range(count):
            total = total + jnp.where(high == j, found[j * cols:(j + 1) * cols], 0.0)
        return total

    def pick_side(i, at):
        return pick(hot_item[i - 1, :, at], lax.div(trip[i:i + 1, at], LOW) - hi_base, by_hi, n_hi)

    n_chunk, per_chunk = trip.shape[1] // PICK, PICK // 128

    def d_send(q):
        @pl.when(q != block)
        def _():
            remote(part_d.at[:, aligned(q * 128, 128, 128)], recv_d.at[block], S_D,
                   emb, lax.rem(q, n_c), lax.div(q, n_c)).start()

    def pick_items(i):
        chunk = lax.rem(lax.div(block, per_chunk) + i, n_chunk)
        at = aligned(chunk * PICK, PICK, 128)
        part_d[:, at] = pick_side(1, at) - pick_side(2, at)
        for j in range(per_chunk):
            d_send(chunk * per_chunk + j)

    each(1, n_chunk + 1, pick_items)
    recv_d[block] = part_d[:, aligned(block * 128, 128, 128)]

    left(mask_bf.at[own_users], S_SWAP)
    either(left, mine, recv_d.at[0:n_in - 1], recv_d.at[0:n_in], S_ITEM0)
    either(left, mine, user0_in.at[0:n_p - 1], user0_in, S_USER0)
    left(deg_item.at[0:n_r - 1], S_DI)
    left(deg_user.at[0:2 * n_c - 1], S_DU)
    for k in range(3):
        left(recv_u.at[k, 0:n_p - 1], S_RU + k)
        left(recv_i.at[k, 0:n_x - 1], S_RI + k)
    left(user1.at[0:n_p - 1], S_GU)
    left(user2.at[0:n_p - 1], S_GU + 1)
    left(item1.at[:, 0:piece * (n_x - 1)], S_GI)
    left(item2.at[:, 0:piece * (n_x - 1)], S_GI + 1)
    either(left, mine, item_own.at[:, 0:sub * (n_e - 1)], item_own, S_OWN)

    either(arrived, fin_mine, fin_all.at[0:n_b - 1], fin_all, S_FIN)
    n_t = n_x * n_c
    here = chip * n_c + lax.div(core * n_c + col, 2)
    wide = jnp.concatenate([fin_all[here], fin_all[n_t + here]], axis=0).astype(F32)
    wide = jnp.where(lax.rem(col, 2) == 1, pltpu.roll(wide, lanes // 2, 1), wide)
    out_user[...] = wide[:, :lanes // 2].astype(BF16)
    by_tile = jnp.concatenate(
        [fin_all[s * n_t + t].astype(F32) for t in range(n_t) for s in range(2)], axis=0).astype(BF16)
    ids = trip[0:1, aligned(block * 128, 128, 128)]
    e_user = pick(one_hot(ids, 128), lax.div(ids, 128), by_tile, n_t)

    arrived(recv_d.at[0:n_b - 1], S_D)
    diff = recv_d[0]
    for i in range(1, n_b):
        diff = diff + recv_d[i]
    zpart[emb] = jnp.sum(e_user * diff, axis=0, keepdims=True)
    for (e_o,) in others(n_e):
        remote(zpart.at[emb], zpart.at[emb], S_Z, e_at[e_o], col, row).start()
    either(left, fin_mine, fin_all.at[0:n_b - 1], fin_all, S_FIN)
    left(recv_d.at[0:n_b - 1], S_D)
    arrived(zpart.at[0:n_e - 1], S_Z)
    score = zpart[0]
    for i in range(1, n_e):
        score = score + zpart[i]
    scores[block] = score
    for x_o, c_o, k_o in others(n_x, n_c, 2):
        remote(scores.at[block], scores.at[block], S_S, emb, c_at[c_o], x_at[x_o] * 2 + k_at[k_o]).start()
    left(zpart.at[0:n_e - 1], S_Z)
    arrived(scores.at[0:n_b - 1], S_S)
    for i in range(n_b):
        score_out[i:i + 1, :] = scores[i]
    left(scores.at[0:n_b - 1], S_S)


def finish(user_in, item_in, score_in, out_user, out_item, loss):
    out_user[...] = user_in[...]
    out_item[...] = item_in[...]
    loss[...] = jax.nn.softplus(-score_in[...])


def solution(mesh):
    dims = n_e, n_c, n_r = mesh.shape["emb"], mesh.shape["col"], mesh.shape["row"]

    def local_fn(mask_blk, user_sh, item_sh, triples):
        rows_u = mask_blk.shape[0]
        width, cols = item_sh.shape
        num_trip = triples.shape[0]
        n_x, n_p, n_b, half = n_r // 2, n_c * n_e, n_r * n_c, n_e // 2
        sub = width // n_e
        ni, cu, kd = n_r * sub, 2 * rows_u, half * cols
        piece, lanes = ni // n_x, cu // n_c
        dma = pltpu.SemaphoreType.DMA
        vmem, hbm = pl.BlockSpec(memory_space=pltpu.VMEM), pl.BlockSpec(memory_space=pltpu.HBM)
        scratch = [
            pltpu.VMEM((cols, user_sh.shape[0]), BF16),
            pltpu.VMEM((8, lanes), BF16),
            pltpu.VMEM((cols, lanes), F32),
            pltpu.VMEM((cols, width), BF16),
            pltpu.VMEM((3, num_trip), I32),
            pltpu.VMEM((n_r, rows_u, sub), I32),
            pltpu.VMEM((n_r, rows_u, width), I32),
            pltpu.VMEM((rows_u, 128), I32),
            pltpu.VMEM((cu, ni), BF16),
            pltpu.VMEM((cu, ni), BF16),
            pltpu.VMEM((n_r, 1, ni), I32),
            pltpu.VMEM((2 * n_c, 1, rows_u), I32),
            pltpu.VMEM((cu, 128), F32),
            pltpu.VMEM((2 * n_c * half, 8, lanes), BF16),
            pltpu.VMEM((kd, cu), F32),
            pltpu.VMEM((kd, ni), BF16),
            pltpu.VMEM((kd, ni), BF16),
            pltpu.VMEM((kd, ni), BF16),
            pltpu.VMEM((n_p, 8, lanes), BF16),
            pltpu.VMEM((n_p, 8, lanes), BF16),
            pltpu.VMEM((3, kd, cu), F32),
            pltpu.VMEM((3, n_p, 8, lanes), F32),
            pltpu.VMEM((3, kd, ni), F32),
            pltpu.VMEM((3, n_x, kd, piece), F32),
            pltpu.VMEM((1, 8, lanes), BF16),
            pltpu.VMEM((kd, piece), BF16),
            pltpu.VMEM((cols, width), BF16),
            pltpu.VMEM((2 * n_x * n_c, 8, lanes), BF16),
            pltpu.VMEM((2, LOW, num_trip), BF16),
            pltpu.VMEM((cols, num_trip), F32),
            pltpu.VMEM((n_b, cols, 128), F32),
            pltpu.VMEM((n_e, 1, 128), F32),
            pltpu.VMEM((n_b, 1, 128), F32),
            dma((n_r,)), dma((n_r,)), dma((3,)), dma((NUM_SEMS,)), dma((NUM_SEMS,)),
        ]
        user_t, item_t, score = pl.pallas_call(
            functools.partial(kernel, dims),
            out_shape=(jax.ShapeDtypeStruct((cols, user_sh.shape[0]), BF16),
                       jax.ShapeDtypeStruct((cols, width), BF16),
                       jax.ShapeDtypeStruct((n_b, 128), F32)),
            in_specs=[hbm, hbm, hbm, hbm],
            out_specs=(vmem, vmem, vmem),
            scratch_shapes=scratch,
            compiler_params=pltpu.CompilerParams(collective_id=0, has_side_effects=True, vmem_limit_bytes=40 << 20),
        )(mask_blk, *(pltpu.with_memory_space_constraint(v.T, pltpu.HBM) for v in (user_sh, item_sh, triples)))
        user_t, item_t, loss = pl.pallas_call(
            finish,
            out_shape=(jax.ShapeDtypeStruct(user_t.shape, BF16), jax.ShapeDtypeStruct(item_t.shape, BF16),
                       jax.ShapeDtypeStruct(score.shape, F32)),
            in_specs=[vmem] * 3,
            compiler_params=pltpu.CompilerParams(vmem_limit_bytes=1 << 20),
        )(user_t, item_t, score)
        return user_t.T, item_t.T, loss.reshape(num_trip)

    return jax.shard_map(
        local_fn, mesh=mesh,
        in_specs=(P("row", "col"), P(("row", "col"), "emb"), P(("col", "row"), "emb"), P()),
        out_specs=(P(("row", "col"), "emb"), P(("col", "row"), "emb"), P()),
        check_vma=False)
```

```python
import functools

import jax
import jax.numpy as jnp
from jax import lax
from jax.experimental import pallas as pl
from jax.experimental.pallas import tpu as pltpu
from jax.sharding import PartitionSpec as P

MESH = pl.DeviceIdType.MESH
F32, BF16, I32 = jnp.float32, jnp.bfloat16, jnp.int32
NUM_LAYERS = 3
CHUNK = 512
PICK = 1024
LOW = 256


def each(lo, hi, body):
    def step(i, carry):
        body(i)
        return carry

    lax.fori_loop(lo, hi, step, 0)


def aligned(start, size, unit):
    return pl.ds(pl.multiple_of(start, unit), size)


def lane_dot(lhs, rhs):
    return lax.dot_general(lhs, rhs, (((1,), (1,)), ((), ())), preferred_element_type=F32)


def far_first(*sizes):
    offsets = [()]
    for n in sizes:
        offsets = [(*o, i) for o in offsets for i in range(n)]
    return sorted(offsets, key=lambda o: -sum(min(i, n - i) for i, n in zip(o, sizes)))


def others(*sizes):
    offsets = [()]
    for n in sizes:
        offsets = [(*o, i) for o in offsets for i in range(n)]
    return offsets[1:]


(S_ITEM0, S_USER0, S_DI, S_DU, S_RU, S_RI, S_GU, S_GI, S_OWN, S_FIN, S_D, S_Z, S_S, S_SWAP, NUM_SEMS) = (
    0, 1, 2, 3, 4, 7, 10, 12, 14, 15, 16, 17, 18, 19, 20)


def kernel(dims, mask_hbm, user_hbm, item_hbm, trip_hbm, out_user, out_item, score_out,
           user_in, user_pack, user_wide, item_in, trip, mask_part, mask_raw, row_acc, mask_bf, adj, deg_item, deg_user, user_scale,
           user0_in, user0, item0, item1, item2,
           user1, user2, part_u, recv_u, part_i, recv_i,
           fin_tile, fin_item, item_own, fin_all, hot_item, part_d, recv_d, zpart, scores,
           sem_part, sem_raw, sem_in, sem_send, sem_recv):
    n_e, n_c, n_r = dims
    n_x, half = n_r // 2, n_e // 2
    n_p = n_c * n_e
    n_b = n_r * n_c
    emb, col, row = lax.axis_index("emb"), lax.axis_index("col"), lax.axis_index("row")
    chip, core = lax.div(row, 2), lax.rem(row, 2)
    rows_u = mask_hbm.shape[0]
    width = item_in.shape[1]
    sub = width // n_e
    cols = item_in.shape[0]
    kd, cu = part_u.shape[1:]
    ni = adj.shape[1]
    piece = ni // n_x
    lanes = cu // n_c
    plane = col * n_e + emb
    block = row * n_c + col
    home = lax.div(emb, half)
    in_half = lax.rem(emb, half)
    mine = home == core
    e_at = [lax.rem(emb + i, n_e) for i in range(n_e)]
    c_at = [lax.rem(col + i, n_c) for i in range(n_c)]
    x_at = [lax.rem(chip + i, n_x) for i in range(n_x)]
    k_at = [core, 1 - core]

    def remote(src, dst, stage, e, c, r):
        return pltpu.make_async_remote_copy(
            src_ref=src, dst_ref=dst, send_sem=sem_send.at[stage], recv_sem=sem_recv.at[stage],
            device_id=(e, c, r), device_id_type=MESH)

    def arrived(view, stage):
        remote(view, view, stage, emb, col, row).wait_recv()

    def left(view, stage):
        remote(view, view, stage, emb, col, row).wait_send()

    def either(wait, alone, less, full, stage):
        @pl.when(alone)
        def _():
            wait(less, stage)

        @pl.when(jnp.logical_not(alone))
        def _():
            wait(full, stage)

    odd = lax.rem(emb, 2)
    n_half = n_r // 2

    def part(i):
        return pltpu.make_async_copy(
            mask_hbm.at[:, aligned(i * width + emb * sub, sub, 128)], mask_part.at[i], sem_part.at[i])

    def raw(i):
        return pltpu.make_async_copy(
            mask_hbm.at[:, aligned((odd * n_half + i) * width, width, 128)], mask_raw.at[i], sem_raw.at[i])

    fetch = [pltpu.make_async_copy(src, dst, sem_in.at[i]) for i, (src, dst) in enumerate(
        ((user_hbm, user_in), (item_hbm, item_in), (trip_hbm, trip)))]

    barrier = pltpu.get_barrier_semaphore()

    def hello(e, c, r):
        pl.semaphore_signal(barrier, inc=1, device_id=(e, c, r), device_id_type=MESH)

    for x_o, e_o, k_o in far_first(n_x, n_e, 2)[:-1]:
        hello(e_at[e_o], col, x_at[x_o] * 2 + k_at[k_o])
    for c_o, e_o, k_o in far_first(n_c, n_e, 2):
        if c_o:
            hello(e_at[e_o], c_at[c_o], chip * 2 + k_at[k_o])
    for copy in fetch:
        copy.start()
    for i in range(n_r):
        part(i).start()

    own_users = aligned(core * rows_u, rows_u, 128)
    for i in range(n_r):
        part(i).wait()
        mask_bf[own_users, i * sub:(i + 1) * sub] = mask_part[i].astype(F32).astype(BF16)
    for i in range(n_half):
        raw(i).start()
    deg_item[row] = jnp.dot(
        jnp.ones((8, rows_u), BF16), mask_bf[own_users, :], preferred_element_type=F32)[0:1].astype(I32)

    fetch[0].wait()
    user_wide[...] = jnp.zeros_like(user_wide)
    user_wide[:, 0:lanes // 2] = user_in[...].astype(F32)
    wide = user_wide[...]
    user_pack[...] = (wide[0:8] + pltpu.roll(wide[8:16], lanes // 2, 1)).astype(BF16)
    fetch[1].wait()
    fetch[2].wait()
    pl.semaphore_wait(barrier, n_r * n_e - 1 + 2 * n_e * (n_c - 1))

    for x_o, k_o in others(n_x, 2):
        remote(deg_item.at[row], deg_item.at[row], S_DI, emb, col, x_at[x_o] * 2 + k_at[k_o]).start()

    here_rows = aligned(in_half * cols, cols, 16)
    here_items = aligned(row * sub, sub, 128)
    user_slot = (core * n_c + col) * half + in_half

    def user0_send(c_o, e_o):
        remote(user_pack, user0_in.at[user_slot], S_USER0, e_at[e_o], c_at[c_o], chip * 2 + home).start()

    for c_o, e_o in others(n_c, n_e):
        user0_send(c_o, e_o)
    remote(mask_bf.at[own_users], mask_bf.at[own_users], S_SWAP, emb, col, chip * 2 + 1 - core).start()

    def item0_send(x_o, e_o):
        remote(item_in.at[:, aligned(e_at[e_o] * sub, sub, 128)], item0.at[here_rows, here_items], S_ITEM0,
               e_at[e_o], col, x_at[x_o] * 2 + home).start()

    for x_o, e_o in others(n_x, n_e):
        item0_send(x_o, e_o)

    @pl.when(jnp.logical_not(mine))
    def _():
        user0_send(0, 0)
        item0_send(0, 0)

    @pl.when(mine)
    def _():
        item0[here_rows, here_items] = item_in[:, aligned(emb * sub, sub, 128)]
        user0_in[user_slot] = user_pack[...]

    for i in range(n_half):
        raw(i).wait()

        def row_sums(t):
            rs = aligned(t * 32, 32, 32)
            total = mask_raw[i, rs, 0:128]
            for j in range(1, width // 128):
                total = total + mask_raw[i, rs, j * 128:(j + 1) * 128]
            row_acc[rs, :] = total if i == 0 else row_acc[rs, :] + total

        each(0, rows_u // 32, row_sums)
    own_part = (core * n_c + col) * 2 + odd
    e_pair = [emb, emb + 1 - 2 * odd]
    deg_user[own_part] = jnp.sum(jnp.transpose(row_acc[...].astype(F32)), axis=0, keepdims=True).astype(I32)
    for c_o, k_o, e_o in others(n_c, 2, 2):
        remote(deg_user.at[own_part], deg_user.at[own_part], S_DU, e_pair[e_o], c_at[c_o], chip * 2 + k_at[k_o]).start()

    def one_hot(ids, size):
        return (lax.broadcasted_iota(I32, (size, ids.shape[1]), 0) == lax.rem(ids, size)).astype(F32).astype(BF16)

    def hot_items(i):
        at = aligned(i * CHUNK, CHUNK, 128)
        for j in range(2):
            hot_item[j, :, at] = one_hot(trip[j + 1:j + 2, at], LOW)

    each(0, trip.shape[1] // CHUNK, hot_items)

    arrived(deg_item.at[0:n_r - 1], S_DI)
    arrived(deg_user.at[0:4 * n_c - 1], S_DU)
    total_i = deg_item[0]
    for i in range(1, n_r):
        total_i = total_i + deg_item[i]
    totals = []
    for k in range(2):
        total = deg_user[k * 2 * n_c]
        for i in range(1, 2 * n_c):
            total = total + deg_user[k * 2 * n_c + i]
        totals.append(total)
    total_u = jnp.concatenate(totals, axis=1)
    inv_item = lax.rsqrt(jnp.maximum(total_i, 1).astype(F32))
    inv_user = lax.rsqrt(jnp.maximum(total_u, 1).astype(F32))
    user_scale[...] = jnp.transpose(jnp.broadcast_to(inv_user, (128, cu)))

    def scale_rows(i):
        rs = aligned(i * 32, 32, 32)
        by_user = user_scale[rs, :]
        for j in range(ni // 128):
            js = slice(j * 128, (j + 1) * 128)
            adj[rs, js] = ((by_user * mask_bf[rs, js].astype(F32)) * inv_item[:, js]).astype(BF16)

    arrived(mask_bf.at[own_users], S_SWAP)
    each(0, cu // 32, scale_rows)

    own_items = aligned(chip * piece, piece, 128)
    own_rows, own_lanes = aligned(emb * 8, 8, 8), aligned(col * lanes, lanes, 128)

    def step_u(k, items):
        pairs = n_c // 2
        mate = lax.rem(col, 2)
        for (p_o,) in far_first(pairs):
            p_to = lax.rem(lax.div(col, 2) + p_o, pairs)
            both = aligned(p_to * 2 * lanes, 2 * lanes, 128)
            part_u[k, :, both] = lane_dot(items, adj[both, :])
            for c_o in (1, 0):
                c_to = p_to * 2 + lax.rem(mate + c_o, 2)
                for (e_o,) in far_first(n_e):
                    tile = part_u.at[k, aligned(e_at[e_o] * 8, 8, 8), aligned(c_to * lanes, lanes, 128)]
                    if p_o or c_o or e_o:
                        remote(tile, recv_u.at[k, plane], S_RU + k, e_at[e_o], c_to, row).start()
                    else:
                        recv_u[k, plane] = tile[...]

    def step_i(k, users):
        for (x_o,) in far_first(n_x):
            there = aligned(x_at[x_o] * piece, piece, 128)
            part = jnp.dot(users, adj[:, there], preferred_element_type=F32)
            if x_o:
                part_i[k, :, there] = part
                remote(part_i.at[k, :, there], recv_i.at[k, chip], S_RI + k, emb, col, x_at[x_o] * 2 + core).start()
            else:
                recv_i[k, chip] = part

    def sum_u(k):
        arrived(recv_u.at[k, 0:n_p - 1], S_RU + k)
        total = recv_u[k, 0]
        for i in range(1, n_p):
            total = total + recv_u[k, i]
        return total.astype(BF16)

    def sum_i(k):
        arrived(recv_i.at[k, 0:n_x - 1], S_RI + k)
        total = recv_i[k, 0]
        for i in range(1, n_x):
            total = total + recv_i[k, i]
        return total.astype(BF16)

    def share_u(buf, k):
        for c_o, e_o in others(n_c, n_e):
            remote(buf.at[plane], buf.at[plane], S_GU + k, e_at[e_o], c_at[c_o], row).start()

    def share_i(buf, k):
        for (x_o,) in others(n_x):
            remote(buf.at[:, own_items], buf.at[:, own_items], S_GI + k, emb, col, x_at[x_o] * 2 + core).start()

    def whole_u(buf, k):
        arrived(buf.at[0:n_p - 1], S_GU + k)
        return jnp.concatenate(
            [jnp.concatenate([buf[c * n_e + e].astype(F32) for c in range(n_c)], axis=1) for e in range(n_e)],
            axis=0).astype(BF16)

    def whole_i(buf, k):
        arrived(buf.at[:, 0:piece * (n_x - 1)], S_GI + k)
        return buf[...]

    either(arrived, mine, user0_in.at[0:n_p - 1], user0_in, S_USER0)
    low = lax.broadcasted_iota(I32, (8, lanes), 1) < lanes // 2
    for t in range(n_c):
        for i in range(half):
            one = user0_in[2 * t * half + i].astype(F32)
            two = user0_in[(2 * t + 1) * half + i].astype(F32)
            ts = slice(t * lanes, (t + 1) * lanes)
            user0[i * cols:i * cols + 8, ts] = jnp.where(low, one, pltpu.roll(two, lanes // 2, 1))
            user0[i * cols + 8:i * cols + 16, ts] = jnp.where(low, pltpu.roll(one, lanes // 2, 1), two)
    step_i(0, user0[...].astype(BF16))
    n_in = n_r * half
    either(arrived, mine, recv_d.at[0:n_in - 1], recv_d.at[0:n_in], S_ITEM0)
    step_u(0, item0[...])

    got = sum_i(0)
    item1[:, own_items] = got
    share_i(item1, 0)
    item_acc = item0[:, own_items].astype(F32) + got.astype(F32)
    got = sum_u(0)
    user1[plane] = got
    share_u(user1, 0)
    user_acc = user0[own_rows, own_lanes] + got.astype(F32)

    step_u(1, whole_i(item1, 0))
    step_i(1, whole_u(user1, 0))
    got = sum_u(1)
    user2[plane] = got
    share_u(user2, 1)
    user_acc = user_acc + got.astype(F32)
    got = sum_i(1)
    item2[:, own_items] = got
    share_i(item2, 1)
    item_acc = item_acc + got.astype(F32)

    step_i(2, whole_u(user2, 1))
    step_u(2, whole_i(item2, 1))

    item_acc = item_acc + sum_i(2).astype(F32)
    fin_item[...] = (item_acc / (NUM_LAYERS + 1)).astype(BF16)
    back = aligned(emb * sub, sub, 128)

    def own_send(e_o, k_o):
        e_to = lax.rem(in_half + e_o, half)
        remote(fin_item.at[aligned(e_to * cols, cols, 16), aligned(k_at[k_o] * sub, sub, 128)], item_own.at[:, back],
               S_OWN, half * core + e_to, col, chip * 2 + k_at[k_o]).start()

    for e_o, k_o in others(half, 2):
        own_send(e_o, k_o)

    @pl.when(jnp.logical_not(mine))
    def _():
        own_send(0, 0)

    @pl.when(mine)
    def _():
        item_own[:, back] = fin_item[here_rows, aligned(core * sub, sub, 128)]

    user_acc = user_acc + sum_u(2).astype(F32)
    fin_tile[0] = (user_acc / (NUM_LAYERS + 1)).astype(BF16)
    e_fin = half * core + lax.div(emb, 2)
    slot = lax.rem(emb, 2) * (n_x * n_c) + chip * n_c + col
    fin_mine = e_fin == emb

    def fin_send(x_o, c_o, k_o):
        remote(fin_tile.at[0], fin_all.at[slot], S_FIN, e_fin, c_at[c_o], x_at[x_o] * 2 + k_at[k_o]).start()

    for offsets in others(n_x, n_c, 2):
        fin_send(*offsets)

    @pl.when(jnp.logical_not(fin_mine))
    def _():
        fin_send(0, 0, 0)

    @pl.when(fin_mine)
    def _():
        fin_all[slot] = fin_tile[0]

    either(arrived, mine, item_own.at[:, 0:sub * (n_e - 1)], item_own, S_OWN)
    out_item[...] = item_own[...]

    n_hi = width // LOW
    by_hi = jnp.concatenate([item_own[:, j * LOW:(j + 1) * LOW] for j in range(n_hi)], axis=0)
    hi_base = (col * n_r + row) * n_hi

    def pick(hot, high, table, count):
        found = jnp.dot(table, hot, preferred_element_type=F32)
        total = jnp.zeros((cols, high.shape[1]), F32)
        for j in range(count):
            total = total + jnp.where(high == j, found[j * cols:(j + 1) * cols], 0.0)
        return total

    def pick_side(i, at):
        return pick(hot_item[i - 1, :, at], lax.div(trip[i:i + 1, at], LOW) - hi_base, by_hi, n_hi)

    n_chunk, per_chunk = trip.shape[1] // PICK, PICK // 128

    def d_send(q):
        @pl.when(q != block)
        def _():
            remote(part_d.at[:, aligned(q * 128, 128, 128)], recv_d.at[block], S_D,
                   emb, lax.rem(q, n_c), lax.div(q, n_c)).start()

    def pick_items(i):
        chunk = lax.rem(lax.div(block, per_chunk) + i, n_chunk)
        at = aligned(chunk * PICK, PICK, 128)
        part_d[:, at] = pick_side(1, at) - pick_side(2, at)
        for j in range(per_chunk):
            d_send(chunk * per_chunk + j)

    for (i,) in far_first(n_chunk):
        pick_items(i)
    recv_d[block] = part_d[:, aligned(block * 128, 128, 128)]

    left(mask_bf.at[own_users], S_SWAP)
    either(left, mine, recv_d.at[0:n_in - 1], recv_d.at[0:n_in], S_ITEM0)
    either(left, mine, user0_in.at[0:n_p - 1], user0_in, S_USER0)
    left(deg_item.at[0:n_r - 1], S_DI)
    left(deg_user.at[0:4 * n_c - 1], S_DU)
    for k in range(3):
        left(recv_u.at[k, 0:n_p - 1], S_RU + k)
        left(recv_i.at[k, 0:n_x - 1], S_RI + k)
    left(user1.at[0:n_p - 1], S_GU)
    left(user2.at[0:n_p - 1], S_GU + 1)
    left(item1.at[:, 0:piece * (n_x - 1)], S_GI)
    left(item2.at[:, 0:piece * (n_x - 1)], S_GI + 1)
    either(left, mine, item_own.at[:, 0:sub * (n_e - 1)], item_own, S_OWN)

    either(arrived, fin_mine, fin_all.at[0:n_b - 1], fin_all, S_FIN)
    n_t = n_x * n_c
    here = chip * n_c + lax.div(core * n_c + col, 2)
    wide = jnp.concatenate([fin_all[here], fin_all[n_t + here]], axis=0).astype(F32)
    wide = jnp.where(lax.rem(col, 2) == 1, pltpu.roll(wide, lanes // 2, 1), wide)
    out_user[...] = wide[:, :lanes // 2].astype(BF16)
    by_tile = jnp.concatenate(
        [fin_all[s * n_t + t].astype(F32) for t in range(n_t) for s in range(2)], axis=0).astype(BF16)
    ids = trip[0:1, aligned(block * 128, 128, 128)]
    e_user = pick(one_hot(ids, 128), lax.div(ids, 128), by_tile, n_t)

    arrived(recv_d.at[0:n_b - 1], S_D)
    diff = recv_d[0]
    for i in range(1, n_b):
        diff = diff + recv_d[i]
    zpart[emb] = jnp.sum(e_user * diff, axis=0, keepdims=True)
    for (e_o,) in others(n_e):
        remote(zpart.at[emb], zpart.at[emb], S_Z, e_at[e_o], col, row).start()
    either(left, fin_mine, fin_all.at[0:n_b - 1], fin_all, S_FIN)
    left(recv_d.at[0:n_b - 1], S_D)
    arrived(zpart.at[0:n_e - 1], S_Z)
    score = zpart[0]
    for i in range(1, n_e):
        score = score + zpart[i]
    scores[block] = score
    for x_o, c_o, k_o in others(n_x, n_c, 2):
        remote(scores.at[block], scores.at[block], S_S, emb, c_at[c_o], x_at[x_o] * 2 + k_at[k_o]).start()
    left(zpart.at[0:n_e - 1], S_Z)
    arrived(scores.at[0:n_b - 1], S_S)
    for i in range(n_b):
        score_out[i:i + 1, :] = scores[i]
    left(scores.at[0:n_b - 1], S_S)


def finish(user_in, item_in, score_in, out_user, out_item, loss):
    out_user[...] = user_in[...]
    out_item[...] = item_in[...]
    loss[...] = jax.nn.softplus(-score_in[...])


def solution(mesh):
    dims = n_e, n_c, n_r = mesh.shape["emb"], mesh.shape["col"], mesh.shape["row"]

    def local_fn(mask_blk, user_sh, item_sh, triples):
        rows_u = mask_blk.shape[0]
        width, cols = item_sh.shape
        num_trip = triples.shape[0]
        n_x, n_p, n_b, half = n_r // 2, n_c * n_e, n_r * n_c, n_e // 2
        sub = width // n_e
        ni, cu, kd = n_r * sub, 2 * rows_u, half * cols
        piece, lanes = ni // n_x, cu // n_c
        dma = pltpu.SemaphoreType.DMA
        vmem, hbm = pl.BlockSpec(memory_space=pltpu.VMEM), pl.BlockSpec(memory_space=pltpu.HBM)
        scratch = [
            pltpu.VMEM((cols, user_sh.shape[0]), BF16),
            pltpu.VMEM((8, lanes), BF16),
            pltpu.VMEM((cols, lanes), F32),
            pltpu.VMEM((cols, width), BF16),
            pltpu.VMEM((3, num_trip), I32),
            pltpu.VMEM((n_r, rows_u, sub), I32),
            pltpu.VMEM((n_x, rows_u, width), I32),
            pltpu.VMEM((rows_u, 128), I32),
            pltpu.VMEM((cu, ni), BF16),
            pltpu.VMEM((cu, ni), BF16),
            pltpu.VMEM((n_r, 1, ni), I32),
            pltpu.VMEM((4 * n_c, 1, rows_u), I32),
            pltpu.VMEM((cu, 128), F32),
            pltpu.VMEM((2 * n_c * half, 8, lanes), BF16),
            pltpu.VMEM((kd, cu), F32),
            pltpu.VMEM((kd, ni), BF16),
            pltpu.VMEM((kd, ni), BF16),
            pltpu.VMEM((kd, ni), BF16),
            pltpu.VMEM((n_p, 8, lanes), BF16),
            pltpu.VMEM((n_p, 8, lanes), BF16),
            pltpu.VMEM((3, kd, cu), F32),
            pltpu.VMEM((3, n_p, 8, lanes), F32),
            pltpu.VMEM((3, kd, ni), F32),
            pltpu.VMEM((3, n_x, kd, piece), F32),
            pltpu.VMEM((1, 8, lanes), BF16),
            pltpu.VMEM((kd, piece), BF16),
            pltpu.VMEM((cols, width), BF16),
            pltpu.VMEM((2 * n_x * n_c, 8, lanes), BF16),
            pltpu.VMEM((2, LOW, num_trip), BF16),
            pltpu.VMEM((cols, num_trip), F32),
            pltpu.VMEM((n_b, cols, 128), F32),
            pltpu.VMEM((n_e, 1, 128), F32),
            pltpu.VMEM((n_b, 1, 128), F32),
            dma((n_r,)), dma((n_r,)), dma((3,)), dma((NUM_SEMS,)), dma((NUM_SEMS,)),
        ]
        user_t, item_t, score = pl.pallas_call(
            functools.partial(kernel, dims),
            out_shape=(jax.ShapeDtypeStruct((cols, user_sh.shape[0]), BF16),
                       jax.ShapeDtypeStruct((cols, width), BF16),
                       jax.ShapeDtypeStruct((n_b, 128), F32)),
            in_specs=[hbm, hbm, hbm, hbm],
            out_specs=(vmem, vmem, vmem),
            scratch_shapes=scratch,
            compiler_params=pltpu.CompilerParams(collective_id=0, has_side_effects=True, vmem_limit_bytes=40 << 20),
        )(mask_blk, *(pltpu.with_memory_space_constraint(v.T, pltpu.HBM) for v in (user_sh, item_sh, triples)))
        user_t, item_t, loss = pl.pallas_call(
            finish,
            out_shape=(jax.ShapeDtypeStruct(user_t.shape, BF16), jax.ShapeDtypeStruct(item_t.shape, BF16),
                       jax.ShapeDtypeStruct(score.shape, F32)),
            in_specs=[vmem] * 3,
            compiler_params=pltpu.CompilerParams(vmem_limit_bytes=1 << 20),
        )(user_t, item_t, score)
        return user_t.T, item_t.T, loss.reshape(num_trip)

    return jax.shard_map(
        local_fn, mesh=mesh,
        in_specs=(P("row", "col"), P(("row", "col"), "emb"), P(("col", "row"), "emb"), P()),
        out_specs=(P(("row", "col"), "emb"), P(("col", "row"), "emb"), P()),
        check_vma=False)
```

```python
import functools

import jax
import jax.numpy as jnp
from jax import lax
from jax.experimental import pallas as pl
from jax.experimental.pallas import tpu as pltpu
from jax.sharding import PartitionSpec as P

MESH = pl.DeviceIdType.MESH
F32, BF16, I32 = jnp.float32, jnp.bfloat16, jnp.int32
NUM_LAYERS = 3
CHUNK = 512
PICK = 1024
LOW = 256


def each(lo, hi, body):
    def step(i, carry):
        body(i)
        return carry

    lax.fori_loop(lo, hi, step, 0)


def aligned(start, size, unit):
    return pl.ds(pl.multiple_of(start, unit), size)


def lane_dot(lhs, rhs):
    return lax.dot_general(lhs, rhs, (((1,), (1,)), ((), ())), preferred_element_type=F32)


def far_first(*sizes):
    offsets = [()]
    for n in sizes:
        offsets = [(*o, i) for o in offsets for i in range(n)]
    return sorted(offsets, key=lambda o: -sum(min(i, n - i) for i, n in zip(o, sizes)))


def others(*sizes):
    offsets = [()]
    for n in sizes:
        offsets = [(*o, i) for o in offsets for i in range(n)]
    return offsets[1:]


(S_ITEM0, S_USER0, S_DI, S_DU, S_RU, S_RI, S_GU, S_GI, S_OWN, S_FIN, S_D, S_Z, S_S, S_SWAP, NUM_SEMS) = (
    0, 1, 2, 3, 4, 7, 10, 12, 14, 15, 16, 17, 18, 19, 20)


def kernel(dims, mask_hbm, user_hbm, item_hbm, trip_hbm, out_user, out_item, score_out,
           user_in, user_pack, user_wide, item_in, trip, mask_part, mask_raw, row_acc, mask_bf, adj, deg_item, deg_user, user_scale,
           user0_in, user0, item0, item1, item2,
           user1, user2, part_u, recv_u, part_i, recv_i,
           fin_tile, fin_item, item_own, fin_all, hot_item, part_d, recv_d, zpart, scores,
           sem_part, sem_raw, sem_in, sem_send, sem_recv):
    n_e, n_c, n_r = dims
    n_x, half = n_r // 2, n_e // 2
    n_p = n_c * n_e
    n_b = n_r * n_c
    emb, col, row = lax.axis_index("emb"), lax.axis_index("col"), lax.axis_index("row")
    chip, core = lax.div(row, 2), lax.rem(row, 2)
    rows_u = mask_hbm.shape[0]
    width = item_in.shape[1]
    sub = width // n_e
    cols = item_in.shape[0]
    kd, cu = part_u.shape[1:]
    ni = adj.shape[1]
    piece = ni // n_x
    lanes = cu // n_c
    plane = col * n_e + emb
    block = row * n_c + col
    home = lax.div(emb, half)
    in_half = lax.rem(emb, half)
    mine = home == core
    e_at = [lax.rem(emb + i, n_e) for i in range(n_e)]
    c_at = [lax.rem(col + i, n_c) for i in range(n_c)]
    x_at = [lax.rem(chip + i, n_x) for i in range(n_x)]
    k_at = [core, 1 - core]

    def remote(src, dst, stage, e, c, r):
        return pltpu.make_async_remote_copy(
            src_ref=src, dst_ref=dst, send_sem=sem_send.at[stage], recv_sem=sem_recv.at[stage],
            device_id=(e, c, r), device_id_type=MESH)

    def arrived(view, stage):
        remote(view, view, stage, emb, col, row).wait_recv()

    def left(view, stage):
        remote(view, view, stage, emb, col, row).wait_send()

    def either(wait, alone, less, full, stage):
        @pl.when(alone)
        def _():
            wait(less, stage)

        @pl.when(jnp.logical_not(alone))
        def _():
            wait(full, stage)

    def part(i):
        return pltpu.make_async_copy(
            mask_hbm.at[:, aligned(i * width + emb * sub, sub, 128)], mask_part.at[i], sem_part.at[i])

    def raw(i):
        return pltpu.make_async_copy(
            mask_hbm.at[:, i * width:(i + 1) * width], mask_raw.at[i], sem_raw.at[i])

    fetch = [pltpu.make_async_copy(src, dst, sem_in.at[i]) for i, (src, dst) in enumerate(
        ((user_hbm, user_in), (item_hbm, item_in), (trip_hbm, trip)))]

    barrier = pltpu.get_barrier_semaphore()

    def hello(e, c, r):
        pl.semaphore_signal(barrier, inc=1, device_id=(e, c, r), device_id_type=MESH)

    for x_o, e_o, k_o in far_first(n_x, n_e, 2)[:-1]:
        hello(e_at[e_o], col, x_at[x_o] * 2 + k_at[k_o])
    for c_o, e_o, k_o in far_first(n_c, n_e, 2):
        if c_o:
            hello(e_at[e_o], c_at[c_o], chip * 2 + k_at[k_o])
    for copy in fetch:
        copy.start()
    for i in range(n_r):
        part(i).start()

    own_users = aligned(core * rows_u, rows_u, 128)
    for i in range(n_r):
        part(i).wait()
        mask_bf[own_users, i * sub:(i + 1) * sub] = mask_part[i].astype(F32).astype(BF16)
    for i in range(n_r):
        raw(i).start()
    deg_item[row] = jnp.dot(
        jnp.ones((8, rows_u), BF16), mask_bf[own_users, :], preferred_element_type=F32)[0:1].astype(I32)

    fetch[0].wait()
    user_wide[...] = jnp.zeros_like(user_wide)
    user_wide[:, 0:lanes // 2] = user_in[...].astype(F32)
    wide = user_wide[...]
    user_pack[...] = (wide[0:8] + pltpu.roll(wide[8:16], lanes // 2, 1)).astype(BF16)
    fetch[1].wait()
    fetch[2].wait()
    pl.semaphore_wait(barrier, n_r * n_e - 1 + 2 * n_e * (n_c - 1))

    for x_o, k_o in others(n_x, 2):
        remote(deg_item.at[row], deg_item.at[row], S_DI, emb, col, x_at[x_o] * 2 + k_at[k_o]).start()

    here_rows = aligned(in_half * cols, cols, 16)
    here_items = aligned(row * sub, sub, 128)
    user_slot = (core * n_c + col) * half + in_half

    def user0_send(c_o, e_o):
        remote(user_pack, user0_in.at[user_slot], S_USER0, e_at[e_o], c_at[c_o], chip * 2 + home).start()

    for c_o, e_o in others(n_c, n_e):
        user0_send(c_o, e_o)
    remote(mask_bf.at[own_users], mask_bf.at[own_users], S_SWAP, emb, col, chip * 2 + 1 - core).start()

    def item0_send(x_o, e_o):
        remote(item_in.at[:, aligned(e_at[e_o] * sub, sub, 128)], item0.at[here_rows, here_items], S_ITEM0,
               e_at[e_o], col, x_at[x_o] * 2 + home).start()

    for x_o, e_o in others(n_x, n_e):
        item0_send(x_o, e_o)

    @pl.when(jnp.logical_not(mine))
    def _():
        user0_send(0, 0)
        item0_send(0, 0)

    @pl.when(mine)
    def _():
        item0[here_rows, here_items] = item_in[:, aligned(emb * sub, sub, 128)]
        user0_in[user_slot] = user_pack[...]

    for i in range(n_r):
        raw(i).wait()

        def row_sums(t):
            rs = aligned(t * 32, 32, 32)
            total = mask_raw[i, rs, 0:128]
            for j in range(1, width // 128):
                total = total + mask_raw[i, rs, j * 128:(j + 1) * 128]
            row_acc[rs, :] = total if i == 0 else row_acc[rs, :] + total

        each(0, rows_u // 32, row_sums)
    own_part = core * n_c + col
    deg_user[own_part] = jnp.sum(jnp.transpose(row_acc[...].astype(F32)), axis=0, keepdims=True).astype(I32)
    for c_o, k_o in others(n_c, 2):
        remote(deg_user.at[own_part], deg_user.at[own_part], S_DU, emb, c_at[c_o], chip * 2 + k_at[k_o]).start()

    def one_hot(ids, size):
        return (lax.broadcasted_iota(I32, (size, ids.shape[1]), 0) == lax.rem(ids, size)).astype(F32).astype(BF16)

    def hot_items(i):
        at = aligned(i * CHUNK, CHUNK, 128)
        for j in range(2):
            hot_item[j, :, at] = one_hot(trip[j + 1:j + 2, at], LOW)

    each(0, trip.shape[1] // CHUNK, hot_items)

    arrived(deg_item.at[0:n_r - 1], S_DI)
    arrived(deg_user.at[0:2 * n_c - 1], S_DU)
    total_i = deg_item[0]
    for i in range(1, n_r):
        total_i = total_i + deg_item[i]
    totals = []
    for k in range(2):
        total = deg_user[k * n_c]
        for i in range(1, n_c):
            total = total + deg_user[k * n_c + i]
        totals.append(total)
    total_u = jnp.concatenate(totals, axis=1)
    inv_item = lax.rsqrt(jnp.maximum(total_i, 1).astype(F32))
    inv_user = lax.rsqrt(jnp.maximum(total_u, 1).astype(F32))
    user_scale[...] = jnp.transpose(jnp.broadcast_to(inv_user, (128, cu)))

    def scale_rows(i):
        rs = aligned(i * 32, 32, 32)
        by_user = user_scale[rs, :]
        for j in range(ni // 128):
            js = slice(j * 128, (j + 1) * 128)
            adj[rs, js] = ((by_user * mask_bf[rs, js].astype(F32)) * inv_item[:, js]).astype(BF16)

    arrived(mask_bf.at[own_users], S_SWAP)
    each(0, cu // 32, scale_rows)

    own_items = aligned(chip * piece, piece, 128)
    own_rows, own_lanes = aligned(emb * 8, 8, 8), aligned(col * lanes, lanes, 128)

    def step_u(k, items):
        pairs = n_c // 2
        mate = lax.rem(col, 2)
        for (p_o,) in far_first(pairs):
            p_to = lax.rem(lax.div(col, 2) + p_o, pairs)
            both = aligned(p_to * 2 * lanes, 2 * lanes, 128)
            part_u[k, :, both] = lane_dot(items, adj[both, :])
            for c_o in (1, 0):
                c_to = p_to * 2 + lax.rem(mate + c_o, 2)
                for (e_o,) in far_first(n_e):
                    tile = part_u.at[k, aligned(e_at[e_o] * 8, 8, 8), aligned(c_to * lanes, lanes, 128)]
                    if p_o or c_o or e_o:
                        remote(tile, recv_u.at[k, plane], S_RU + k, e_at[e_o], c_to, row).start()
                    else:
                        recv_u[k, plane] = tile[...]

    def step_i(k, users):
        for (x_o,) in far_first(n_x):
            there = aligned(x_at[x_o] * piece, piece, 128)
            part = jnp.dot(users, adj[:, there], preferred_element_type=F32)
            if x_o:
                part_i[k, :, there] = part
                remote(part_i.at[k, :, there], recv_i.at[k, chip], S_RI + k, emb, col, x_at[x_o] * 2 + core).start()
            else:
                recv_i[k, chip] = part

    def sum_u(k):
        arrived(recv_u.at[k, 0:n_p - 1], S_RU + k)
        total = recv_u[k, 0]
        for i in range(1, n_p):
            total = total + recv_u[k, i]
        return total.astype(BF16)

    def sum_i(k):
        arrived(recv_i.at[k, 0:n_x - 1], S_RI + k)
        total = recv_i[k, 0]
        for i in range(1, n_x):
            total = total + recv_i[k, i]
        return total.astype(BF16)

    def share_u(buf, k):
        for c_o, e_o in others(n_c, n_e):
            remote(buf.at[plane], buf.at[plane], S_GU + k, e_at[e_o], c_at[c_o], row).start()

    def share_i(buf, k):
        for (x_o,) in others(n_x):
            remote(buf.at[:, own_items], buf.at[:, own_items], S_GI + k, emb, col, x_at[x_o] * 2 + core).start()

    def whole_u(buf, k):
        arrived(buf.at[0:n_p - 1], S_GU + k)
        return jnp.concatenate(
            [jnp.concatenate([buf[c * n_e + e].astype(F32) for c in range(n_c)], axis=1) for e in range(n_e)],
            axis=0).astype(BF16)

    def whole_i(buf, k):
        arrived(buf.at[:, 0:piece * (n_x - 1)], S_GI + k)
        return buf[...]

    either(arrived, mine, user0_in.at[0:n_p - 1], user0_in, S_USER0)
    low = lax.broadcasted_iota(I32, (8, lanes), 1) < lanes // 2
    for t in range(n_c):
        for i in range(half):
            one = user0_in[2 * t * half + i].astype(F32)
            two = user0_in[(2 * t + 1) * half + i].astype(F32)
            ts = slice(t * lanes, (t + 1) * lanes)
            user0[i * cols:i * cols + 8, ts] = jnp.where(low, one, pltpu.roll(two, lanes // 2, 1))
            user0[i * cols + 8:i * cols + 16, ts] = jnp.where(low, pltpu.roll(one, lanes // 2, 1), two)
    step_i(0, user0[...].astype(BF16))
    n_in = n_r * half
    either(arrived, mine, recv_d.at[0:n_in - 1], recv_d.at[0:n_in], S_ITEM0)
    step_u(0, item0[...])

    got = sum_i(0)
    item1[:, own_items] = got
    share_i(item1, 0)
    item_acc = item0[:, own_items].astype(F32) + got.astype(F32)
    got = sum_u(0)
    user1[plane] = got
    share_u(user1, 0)
    user_acc = user0[own_rows, own_lanes] + got.astype(F32)

    step_u(1, whole_i(item1, 0))
    step_i(1, whole_u(user1, 0))
    got = sum_u(1)
    user2[plane] = got
    share_u(user2, 1)
    user_acc = user_acc + got.astype(F32)
    got = sum_i(1)
    item2[:, own_items] = got
    share_i(item2, 1)
    item_acc = item_acc + got.astype(F32)

    step_i(2, whole_u(user2, 1))
    step_u(2, whole_i(item2, 1))

    item_acc = item_acc + sum_i(2).astype(F32)
    fin_item[...] = (item_acc / (NUM_LAYERS + 1)).astype(BF16)
    back = aligned(emb * sub, sub, 128)

    def own_send(e_o, k_o):
        e_to = lax.rem(in_half + e_o, half)
        remote(fin_item.at[aligned(e_to * cols, cols, 16), aligned(k_at[k_o] * sub, sub, 128)], item_own.at[:, back],
               S_OWN, half * core + e_to, col, chip * 2 + k_at[k_o]).start()

    for e_o, k_o in others(half, 2):
        own_send(e_o, k_o)

    @pl.when(jnp.logical_not(mine))
    def _():
        own_send(0, 0)

    @pl.when(mine)
    def _():
        item_own[:, back] = fin_item[here_rows, aligned(core * sub, sub, 128)]

    user_acc = user_acc + sum_u(2).astype(F32)
    fin_tile[0] = (user_acc / (NUM_LAYERS + 1)).astype(BF16)
    e_fin = half * core + lax.div(emb, 2)
    slot = lax.rem(emb, 2) * (n_x * n_c) + chip * n_c + col
    fin_mine = e_fin == emb

    def fin_send(x_o, c_o, k_o):
        remote(fin_tile.at[0], fin_all.at[slot], S_FIN, e_fin, c_at[c_o], x_at[x_o] * 2 + k_at[k_o]).start()

    for offsets in others(n_x, n_c, 2):
        fin_send(*offsets)

    @pl.when(jnp.logical_not(fin_mine))
    def _():
        fin_send(0, 0, 0)

    @pl.when(fin_mine)
    def _():
        fin_all[slot] = fin_tile[0]

    either(arrived, mine, item_own.at[:, 0:sub * (n_e - 1)], item_own, S_OWN)
    out_item[...] = item_own[...]

    n_hi = width // LOW
    by_hi = jnp.concatenate([item_own[:, j * LOW:(j + 1) * LOW] for j in range(n_hi)], axis=0)
    hi_base = (col * n_r + row) * n_hi

    def pick(hot, high, table, count):
        found = jnp.dot(table, hot, preferred_element_type=F32)
        total = jnp.zeros((cols, high.shape[1]), F32)
        for j in range(count):
            total = total + jnp.where(high == j, found[j * cols:(j + 1) * cols], 0.0)
        return total

    def pick_side(i, at):
        return pick(hot_item[i - 1, :, at], lax.div(trip[i:i + 1, at], LOW) - hi_base, by_hi, n_hi)

    n_chunk, per_chunk = trip.shape[1] // PICK, PICK // 128

    def d_send(q):
        @pl.when(q != block)
        def _():
            remote(part_d.at[:, aligned(q * 128, 128, 128)], recv_d.at[block], S_D,
                   emb, lax.rem(q, n_c), lax.div(q, n_c)).start()

    def pick_items(i):
        chunk = lax.rem(lax.div(block, per_chunk) + i, n_chunk)
        at = aligned(chunk * PICK, PICK, 128)
        part_d[:, at] = pick_side(1, at) - pick_side(2, at)
        for j in range(per_chunk):
            d_send(chunk * per_chunk + j)

    for (i,) in far_first(n_chunk):
        pick_items(i)
    recv_d[block] = part_d[:, aligned(block * 128, 128, 128)]

    left(mask_bf.at[own_users], S_SWAP)
    either(left, mine, recv_d.at[0:n_in - 1], recv_d.at[0:n_in], S_ITEM0)
    either(left, mine, user0_in.at[0:n_p - 1], user0_in, S_USER0)
    left(deg_item.at[0:n_r - 1], S_DI)
    left(deg_user.at[0:2 * n_c - 1], S_DU)
    for k in range(3):
        left(recv_u.at[k, 0:n_p - 1], S_RU + k)
        left(recv_i.at[k, 0:n_x - 1], S_RI + k)
    left(user1.at[0:n_p - 1], S_GU)
    left(user2.at[0:n_p - 1], S_GU + 1)
    left(item1.at[:, 0:piece * (n_x - 1)], S_GI)
    left(item2.at[:, 0:piece * (n_x - 1)], S_GI + 1)
    either(left, mine, item_own.at[:, 0:sub * (n_e - 1)], item_own, S_OWN)

    either(arrived, fin_mine, fin_all.at[0:n_b - 1], fin_all, S_FIN)
    n_t = n_x * n_c
    here = chip * n_c + lax.div(core * n_c + col, 2)
    wide = jnp.concatenate([fin_all[here], fin_all[n_t + here]], axis=0).astype(F32)
    wide = jnp.where(lax.rem(col, 2) == 1, pltpu.roll(wide, lanes // 2, 1), wide)
    out_user[...] = wide[:, :lanes // 2].astype(BF16)
    by_tile = jnp.concatenate(
        [fin_all[s * n_t + t].astype(F32) for t in range(n_t) for s in range(2)], axis=0).astype(BF16)
    ids = trip[0:1, aligned(block * 128, 128, 128)]
    e_user = pick(one_hot(ids, 128), lax.div(ids, 128), by_tile, n_t)

    arrived(recv_d.at[0:n_b - 1], S_D)
    diff = recv_d[0]
    for i in range(1, n_b):
        diff = diff + recv_d[i]
    zpart[emb] = jnp.sum(e_user * diff, axis=0, keepdims=True)
    for (e_o,) in others(n_e):
        remote(zpart.at[emb], zpart.at[emb], S_Z, e_at[e_o], col, row).start()
    either(left, fin_mine, fin_all.at[0:n_b - 1], fin_all, S_FIN)
    left(recv_d.at[0:n_b - 1], S_D)
    arrived(zpart.at[0:n_e - 1], S_Z)
    score = zpart[0]
    for i in range(1, n_e):
        score = score + zpart[i]
    scores[block] = score
    for x_o, c_o, k_o in others(n_x, n_c, 2):
        remote(scores.at[block], scores.at[block], S_S, emb, c_at[c_o], x_at[x_o] * 2 + k_at[k_o]).start()
    left(zpart.at[0:n_e - 1], S_Z)
    arrived(scores.at[0:n_b - 1], S_S)
    for i in range(n_b):
        score_out[i:i + 1, :] = scores[i]
    left(scores.at[0:n_b - 1], S_S)


def finish(user_in, item_in, score_in, out_user, out_item, loss):
    out_user[...] = user_in[...]
    out_item[...] = item_in[...]
    loss[...] = jax.nn.softplus(-score_in[...])


def solution(mesh):
    dims = n_e, n_c, n_r = mesh.shape["emb"], mesh.shape["col"], mesh.shape["row"]

    def local_fn(mask_blk, user_sh, item_sh, triples):
        rows_u = mask_blk.shape[0]
        width, cols = item_sh.shape
        num_trip = triples.shape[0]
        n_x, n_p, n_b, half = n_r // 2, n_c * n_e, n_r * n_c, n_e // 2
        sub = width // n_e
        ni, cu, kd = n_r * sub, 2 * rows_u, half * cols
        piece, lanes = ni // n_x, cu // n_c
        dma = pltpu.SemaphoreType.DMA
        vmem, hbm = pl.BlockSpec(memory_space=pltpu.VMEM), pl.BlockSpec(memory_space=pltpu.HBM)
        scratch = [
            pltpu.VMEM((cols, user_sh.shape[0]), BF16),
            pltpu.VMEM((8, lanes), BF16),
            pltpu.VMEM((cols, lanes), F32),
            pltpu.VMEM((cols, width), BF16),
            pltpu.VMEM((3, num_trip), I32),
            pltpu.VMEM((n_r, rows_u, sub), I32),
            pltpu.VMEM((n_r, rows_u, width), I32),
            pltpu.VMEM((rows_u, 128), I32),
            pltpu.VMEM((cu, ni), BF16),
            pltpu.VMEM((cu, ni), BF16),
            pltpu.VMEM((n_r, 1, ni), I32),
            pltpu.VMEM((2 * n_c, 1, rows_u), I32),
            pltpu.VMEM((cu, 128), F32),
            pltpu.VMEM((2 * n_c * half, 8, lanes), BF16),
            pltpu.VMEM((kd, cu), F32),
            pltpu.VMEM((kd, ni), BF16),
            pltpu.VMEM((kd, ni), BF16),
            pltpu.VMEM((kd, ni), BF16),
            pltpu.VMEM((n_p, 8, lanes), BF16),
            pltpu.VMEM((n_p, 8, lanes), BF16),
            pltpu.VMEM((3, kd, cu), F32),
            pltpu.VMEM((3, n_p, 8, lanes), F32),
            pltpu.VMEM((3, kd, ni), F32),
            pltpu.VMEM((3, n_x, kd, piece), F32),
            pltpu.VMEM((1, 8, lanes), BF16),
            pltpu.VMEM((kd, piece), BF16),
            pltpu.VMEM((cols, width), BF16),
            pltpu.VMEM((2 * n_x * n_c, 8, lanes), BF16),
            pltpu.VMEM((2, LOW, num_trip), BF16),
            pltpu.VMEM((cols, num_trip), F32),
            pltpu.VMEM((n_b, cols, 128), F32),
            pltpu.VMEM((n_e, 1, 128), F32),
            pltpu.VMEM((n_b, 1, 128), F32),
            dma((n_r,)), dma((n_r,)), dma((3,)), dma((NUM_SEMS,)), dma((NUM_SEMS,)),
        ]
        user_t, item_t, score = pl.pallas_call(
            functools.partial(kernel, dims),
            out_shape=(jax.ShapeDtypeStruct((cols, user_sh.shape[0]), BF16),
                       jax.ShapeDtypeStruct((cols, width), BF16),
                       jax.ShapeDtypeStruct((n_b, 128), F32)),
            in_specs=[hbm, hbm, hbm, hbm],
            out_specs=(vmem, vmem, vmem),
            scratch_shapes=scratch,
            compiler_params=pltpu.CompilerParams(collective_id=0, has_side_effects=True, vmem_limit_bytes=40 << 20),
        )(mask_blk, *(pltpu.with_memory_space_constraint(v.T, pltpu.HBM) for v in (user_sh, item_sh, triples)))
        user_t, item_t, loss = pl.pallas_call(
            finish,
            out_shape=(jax.ShapeDtypeStruct(user_t.shape, BF16), jax.ShapeDtypeStruct(item_t.shape, BF16),
                       jax.ShapeDtypeStruct(score.shape, F32)),
            in_specs=[vmem] * 3,
            compiler_params=pltpu.CompilerParams(vmem_limit_bytes=1 << 20),
        )(user_t, item_t, score)
        return user_t.T, item_t.T, loss.reshape(num_trip)

    return jax.shard_map(
        local_fn, mesh=mesh,
        in_specs=(P("row", "col"), P(("row", "col"), "emb"), P(("col", "row"), "emb"), P()),
        out_specs=(P(("row", "col"), "emb"), P(("col", "row"), "emb"), P()),
        check_vma=False)
```

```python
import functools

import jax
import jax.numpy as jnp
from jax import lax
from jax.experimental import pallas as pl
from jax.experimental.pallas import tpu as pltpu
from jax.sharding import PartitionSpec as P

MESH = pl.DeviceIdType.MESH
F32, BF16, I32 = jnp.float32, jnp.bfloat16, jnp.int32
NUM_LAYERS = 3
CHUNK = 512
PICK = 1024
LOW = 256


def each(lo, hi, body):
    def step(i, carry):
        body(i)
        return carry

    lax.fori_loop(lo, hi, step, 0)


def aligned(start, size, unit):
    return pl.ds(pl.multiple_of(start, unit), size)


def lane_dot(lhs, rhs):
    return lax.dot_general(lhs, rhs, (((1,), (1,)), ((), ())), preferred_element_type=F32)


def far_first(*sizes):
    offsets = [()]
    for n in sizes:
        offsets = [(*o, i) for o in offsets for i in range(n)]
    return sorted(offsets, key=lambda o: -sum(min(i, n - i) for i, n in zip(o, sizes)))


def others(*sizes):
    offsets = [()]
    for n in sizes:
        offsets = [(*o, i) for o in offsets for i in range(n)]
    return offsets[1:]


(S_ITEM0, S_USER0, S_DI, S_DU, S_RU, S_RI, S_GU, S_GI, S_OWN, S_FIN, S_D, S_Z, S_S, S_SWAP, NUM_SEMS) = (
    0, 1, 2, 3, 4, 7, 10, 12, 14, 15, 16, 17, 18, 19, 20)


def kernel(dims, mask_hbm, user_hbm, item_hbm, trip_hbm, out_user, out_item, score_out,
           user_in, user_pack, user_wide, item_in, trip, mask_part, mask_raw, row_acc, mask_bf, adj, deg_item, deg_user, user_scale,
           user0_in, user0, item0, item1, item2,
           user1, user2, part_u, recv_u, part_i, recv_i,
           fin_tile, fin_item, item_own, fin_all, hot_item, part_d, recv_d, zpart, scores,
           sem_part, sem_raw, sem_in, sem_send, sem_recv):
    n_e, n_c, n_r = dims
    n_x, half = n_r // 2, n_e // 2
    n_p = n_c * n_e
    n_b = n_r * n_c
    emb, col, row = lax.axis_index("emb"), lax.axis_index("col"), lax.axis_index("row")
    chip, core = lax.div(row, 2), lax.rem(row, 2)
    rows_u = mask_hbm.shape[0]
    width = item_in.shape[1]
    sub = width // n_e
    cols = item_in.shape[0]
    kd, cu = part_u.shape[1:]
    ni = adj.shape[1]
    piece = ni // n_x
    lanes = cu // n_c
    plane = col * n_e + emb
    block = row * n_c + col
    home = lax.div(emb, half)
    in_half = lax.rem(emb, half)
    mine = home == core
    e_at = [lax.rem(emb + i, n_e) for i in range(n_e)]
    c_at = [lax.rem(col + i, n_c) for i in range(n_c)]
    x_at = [lax.rem(chip + i, n_x) for i in range(n_x)]
    k_at = [core, 1 - core]

    def remote(src, dst, stage, e, c, r):
        return pltpu.make_async_remote_copy(
            src_ref=src, dst_ref=dst, send_sem=sem_send.at[stage], recv_sem=sem_recv.at[stage],
            device_id=(e, c, r), device_id_type=MESH)

    def arrived(view, stage):
        remote(view, view, stage, emb, col, row).wait_recv()

    def left(view, stage):
        remote(view, view, stage, emb, col, row).wait_send()

    def either(wait, alone, less, full, stage):
        @pl.when(alone)
        def _():
            wait(less, stage)

        @pl.when(jnp.logical_not(alone))
        def _():
            wait(full, stage)

    def part(i):
        return pltpu.make_async_copy(
            mask_hbm.at[:, aligned(i * width + emb * sub, sub, 128)], mask_part.at[i], sem_part.at[i])

    def raw(i):
        return pltpu.make_async_copy(
            mask_hbm.at[:, i * width:(i + 1) * width], mask_raw.at[i], sem_raw.at[i])

    fetch = [pltpu.make_async_copy(src, dst, sem_in.at[i]) for i, (src, dst) in enumerate(
        ((user_hbm, user_in), (item_hbm, item_in), (trip_hbm, trip)))]

    for copy in fetch:
        copy.start()
    for i in range(n_r):
        part(i).start()

    barrier = pltpu.get_barrier_semaphore()

    def hello(e, c, r):
        pl.semaphore_signal(barrier, inc=1, device_id=(e, c, r), device_id_type=MESH)

    for x_o, e_o, k_o in far_first(n_x, n_e, 2)[:-1]:
        hello(e_at[e_o], col, x_at[x_o] * 2 + k_at[k_o])
    for c_o, e_o, k_o in far_first(n_c, n_e, 2):
        if c_o:
            hello(e_at[e_o], c_at[c_o], chip * 2 + k_at[k_o])

    own_users = aligned(core * rows_u, rows_u, 128)
    for i in range(n_r):
        part(i).wait()
    for i in range(n_r):
        raw(i).start()

    fetch[0].wait()
    user_wide[...] = jnp.zeros_like(user_wide)
    user_wide[:, 0:lanes // 2] = user_in[...].astype(F32)
    wide = user_wide[...]
    user_pack[...] = (wide[0:8] + pltpu.roll(wide[8:16], lanes // 2, 1)).astype(BF16)
    fetch[1].wait()
    fetch[2].wait()
    pl.semaphore_wait(barrier, n_r * n_e - 1 + 2 * n_e * (n_c - 1))

    here_rows = aligned(in_half * cols, cols, 16)
    here_items = aligned(row * sub, sub, 128)
    user_slot = (core * n_c + col) * half + in_half

    def user0_send(c_o, e_o):
        remote(user_pack, user0_in.at[user_slot], S_USER0, e_at[e_o], c_at[c_o], chip * 2 + home).start()

    for c_o, e_o in others(n_c, n_e):
        user0_send(c_o, e_o)
    def item0_send(x_o, e_o):
        remote(item_in.at[:, aligned(e_at[e_o] * sub, sub, 128)], item0.at[here_rows, here_items], S_ITEM0,
               e_at[e_o], col, x_at[x_o] * 2 + home).start()

    for x_o, e_o in others(n_x, n_e):
        item0_send(x_o, e_o)

    @pl.when(jnp.logical_not(mine))
    def _():
        user0_send(0, 0)
        item0_send(0, 0)

    @pl.when(mine)
    def _():
        item0[here_rows, here_items] = item_in[:, aligned(emb * sub, sub, 128)]
        user0_in[user_slot] = user_pack[...]

    for i in range(n_r):
        mask_bf[own_users, i * sub:(i + 1) * sub] = mask_part[i].astype(F32).astype(BF16)
    deg_item[row] = jnp.dot(
        jnp.ones((8, rows_u), BF16), mask_bf[own_users, :], preferred_element_type=F32)[0:1].astype(I32)

    for x_o, k_o in others(n_x, 2):
        remote(deg_item.at[row], deg_item.at[row], S_DI, emb, col, x_at[x_o] * 2 + k_at[k_o]).start()

    remote(mask_bf.at[own_users], mask_bf.at[own_users], S_SWAP, emb, col, chip * 2 + 1 - core).start()

    for i in range(n_r):
        raw(i).wait()

        def row_sums(t):
            rs = aligned(t * 32, 32, 32)
            total = mask_raw[i, rs, 0:128]
            for j in range(1, width // 128):
                total = total + mask_raw[i, rs, j * 128:(j + 1) * 128]
            row_acc[rs, :] = total if i == 0 else row_acc[rs, :] + total

        each(0, rows_u // 32, row_sums)
    own_part = core * n_c + col
    deg_user[own_part] = jnp.sum(jnp.transpose(row_acc[...].astype(F32)), axis=0, keepdims=True).astype(I32)
    for c_o, k_o in others(n_c, 2):
        remote(deg_user.at[own_part], deg_user.at[own_part], S_DU, emb, c_at[c_o], chip * 2 + k_at[k_o]).start()

    def one_hot(ids, size):
        return (lax.broadcasted_iota(I32, (size, ids.shape[1]), 0) == lax.rem(ids, size)).astype(F32).astype(BF16)

    def hot_items(i):
        at = aligned(i * CHUNK, CHUNK, 128)
        for j in range(2):
            hot_item[j, :, at] = one_hot(trip[j + 1:j + 2, at], LOW)

    each(0, trip.shape[1] // CHUNK, hot_items)

    arrived(deg_item.at[0:n_r - 1], S_DI)
    arrived(deg_user.at[0:2 * n_c - 1], S_DU)
    total_i = deg_item[0]
    for i in range(1, n_r):
        total_i = total_i + deg_item[i]
    totals = []
    for k in range(2):
        total = deg_user[k * n_c]
        for i in range(1, n_c):
            total = total + deg_user[k * n_c + i]
        totals.append(total)
    total_u = jnp.concatenate(totals, axis=1)
    inv_item = lax.rsqrt(jnp.maximum(total_i, 1).astype(F32))
    inv_user = lax.rsqrt(jnp.maximum(total_u, 1).astype(F32))
    user_scale[...] = jnp.transpose(jnp.broadcast_to(inv_user, (128, cu)))

    def scale_rows(i):
        rs = aligned(i * 32, 32, 32)
        by_user = user_scale[rs, :]
        for j in range(ni // 128):
            js = slice(j * 128, (j + 1) * 128)
            adj[rs, js] = ((by_user * mask_bf[rs, js].astype(F32)) * inv_item[:, js]).astype(BF16)

    arrived(mask_bf.at[own_users], S_SWAP)
    each(0, cu // 32, scale_rows)

    own_items = aligned(chip * piece, piece, 128)
    own_rows, own_lanes = aligned(emb * 8, 8, 8), aligned(col * lanes, lanes, 128)

    def step_u(k, items):
        pairs = n_c // 2
        mate = lax.rem(col, 2)
        for (p_o,) in far_first(pairs):
            p_to = lax.rem(lax.div(col, 2) + p_o, pairs)
            both = aligned(p_to * 2 * lanes, 2 * lanes, 128)
            part_u[k, :, both] = lane_dot(items, adj[both, :])
            for c_o in (1, 0):
                c_to = p_to * 2 + lax.rem(mate + c_o, 2)
                for (e_o,) in far_first(n_e):
                    tile = part_u.at[k, aligned(e_at[e_o] * 8, 8, 8), aligned(c_to * lanes, lanes, 128)]
                    if p_o or c_o or e_o:
                        remote(tile, recv_u.at[k, plane], S_RU + k, e_at[e_o], c_to, row).start()
                    else:
                        recv_u[k, plane] = tile[...]

    def step_i(k, users):
        for (x_o,) in (*others(n_x), (0,)):
            there = aligned(x_at[x_o] * piece, piece, 128)
            part = jnp.dot(users, adj[:, there], preferred_element_type=F32)
            if x_o:
                part_i[k, :, there] = part
                remote(part_i.at[k, :, there], recv_i.at[k, chip], S_RI + k, emb, col, x_at[x_o] * 2 + core).start()
            else:
                recv_i[k, chip] = part

    def sum_u(k):
        arrived(recv_u.at[k, 0:n_p - 1], S_RU + k)
        total = recv_u[k, 0]
        for i in range(1, n_p):
            total = total + recv_u[k, i]
        return total.astype(BF16)

    def sum_i(k):
        arrived(recv_i.at[k, 0:n_x - 1], S_RI + k)
        total = recv_i[k, 0]
        for i in range(1, n_x):
            total = total + recv_i[k, i]
        return total.astype(BF16)

    def share_u(buf, k):
        for c_o, e_o in others(n_c, n_e):
            remote(buf.at[plane], buf.at[plane], S_GU + k, e_at[e_o], c_at[c_o], row).start()

    def share_i(buf, k):
        for (x_o,) in others(n_x):
            remote(buf.at[:, own_items], buf.at[:, own_items], S_GI + k, emb, col, x_at[x_o] * 2 + core).start()

    def whole_u(buf, k):
        arrived(buf.at[0:n_p - 1], S_GU + k)
        return jnp.concatenate(
            [jnp.concatenate([buf[c * n_e + e].astype(F32) for c in range(n_c)], axis=1) for e in range(n_e)],
            axis=0).astype(BF16)

    def whole_i(buf, k):
        arrived(buf.at[:, 0:piece * (n_x - 1)], S_GI + k)
        return buf[...]

    either(arrived, mine, user0_in.at[0:n_p - 1], user0_in, S_USER0)
    low = lax.broadcasted_iota(I32, (8, lanes), 1) < lanes // 2
    for t in range(n_c):
        for i in range(half):
            one = user0_in[2 * t * half + i].astype(F32)
            two = user0_in[(2 * t + 1) * half + i].astype(F32)
            ts = slice(t * lanes, (t + 1) * lanes)
            user0[i * cols:i * cols + 8, ts] = jnp.where(low, one, pltpu.roll(two, lanes // 2, 1))
            user0[i * cols + 8:i * cols + 16, ts] = jnp.where(low, pltpu.roll(one, lanes // 2, 1), two)
    step_i(0, user0[...].astype(BF16))
    n_in = n_r * half
    either(arrived, mine, recv_d.at[0:n_in - 1], recv_d.at[0:n_in], S_ITEM0)
    step_u(0, item0[...])

    got = sum_i(0)
    item1[:, own_items] = got
    share_i(item1, 0)
    item_acc = item0[:, own_items].astype(F32) + got.astype(F32)
    got = sum_u(0)
    user1[plane] = got
    share_u(user1, 0)
    user_acc = user0[own_rows, own_lanes] + got.astype(F32)

    step_u(1, whole_i(item1, 0))
    step_i(1, whole_u(user1, 0))
    got = sum_u(1)
    user2[plane] = got
    share_u(user2, 1)
    user_acc = user_acc + got.astype(F32)
    got = sum_i(1)
    item2[:, own_items] = got
    share_i(item2, 1)
    item_acc = item_acc + got.astype(F32)

    step_i(2, whole_u(user2, 1))
    step_u(2, whole_i(item2, 1))

    item_acc = item_acc + sum_i(2).astype(F32)
    fin_item[...] = (item_acc / (NUM_LAYERS + 1)).astype(BF16)
    back = aligned(emb * sub, sub, 128)

    def own_send(e_o, k_o):
        e_to = lax.rem(in_half + e_o, half)
        remote(fin_item.at[aligned(e_to * cols, cols, 16), aligned(k_at[k_o] * sub, sub, 128)], item_own.at[:, back],
               S_OWN, half * core + e_to, col, chip * 2 + k_at[k_o]).start()

    for e_o, k_o in others(half, 2):
        own_send(e_o, k_o)

    @pl.when(jnp.logical_not(mine))
    def _():
        own_send(0, 0)

    @pl.when(mine)
    def _():
        item_own[:, back] = fin_item[here_rows, aligned(core * sub, sub, 128)]

    user_acc = user_acc + sum_u(2).astype(F32)
    fin_tile[0] = (user_acc / (NUM_LAYERS + 1)).astype(BF16)
    e_fin = half * core + lax.div(emb, 2)
    slot = lax.rem(emb, 2) * (n_x * n_c) + chip * n_c + col
    fin_mine = e_fin == emb

    def fin_send(x_o, c_o, k_o):
        remote(fin_tile.at[0], fin_all.at[slot], S_FIN, e_fin, c_at[c_o], x_at[x_o] * 2 + k_at[k_o]).start()

    for offsets in others(n_x, n_c, 2):
        fin_send(*offsets)

    @pl.when(jnp.logical_not(fin_mine))
    def _():
        fin_send(0, 0, 0)

    @pl.when(fin_mine)
    def _():
        fin_all[slot] = fin_tile[0]

    either(arrived, mine, item_own.at[:, 0:sub * (n_e - 1)], item_own, S_OWN)
    out_item[...] = item_own[...]

    n_hi = width // LOW
    by_hi = jnp.concatenate([item_own[:, j * LOW:(j + 1) * LOW] for j in range(n_hi)], axis=0)
    hi_base = (col * n_r + row) * n_hi

    def pick(hot, high, table, count):
        found = jnp.dot(table, hot, preferred_element_type=F32)
        total = jnp.zeros((cols, high.shape[1]), F32)
        for j in range(count):
            total = total + jnp.where(high == j, found[j * cols:(j + 1) * cols], 0.0)
        return total

    def pick_side(i, at):
        return pick(hot_item[i - 1, :, at], lax.div(trip[i:i + 1, at], LOW) - hi_base, by_hi, n_hi)

    n_chunk, per_chunk = trip.shape[1] // PICK, PICK // 128

    def d_send(q):
        @pl.when(q != block)
        def _():
            remote(part_d.at[:, aligned(q * 128, 128, 128)], recv_d.at[block], S_D,
                   emb, lax.rem(q, n_c), lax.div(q, n_c)).start()

    def pick_items(i):
        chunk = lax.rem(lax.div(block, per_chunk) + i, n_chunk)
        at = aligned(chunk * PICK, PICK, 128)
        part_d[:, at] = pick_side(1, at) - pick_side(2, at)
        for j in range(per_chunk):
            d_send(chunk * per_chunk + j)

    for (i,) in far_first(n_chunk):
        pick_items(i)
    recv_d[block] = part_d[:, aligned(block * 128, 128, 128)]

    left(mask_bf.at[own_users], S_SWAP)
    either(left, mine, recv_d.at[0:n_in - 1], recv_d.at[0:n_in], S_ITEM0)
    either(left, mine, user0_in.at[0:n_p - 1], user0_in, S_USER0)
    left(deg_item.at[0:n_r - 1], S_DI)
    left(deg_user.at[0:2 * n_c - 1], S_DU)
    for k in range(3):
        left(recv_u.at[k, 0:n_p - 1], S_RU + k)
        left(recv_i.at[k, 0:n_x - 1], S_RI + k)
    left(user1.at[0:n_p - 1], S_GU)
    left(user2.at[0:n_p - 1], S_GU + 1)
    left(item1.at[:, 0:piece * (n_x - 1)], S_GI)
    left(item2.at[:, 0:piece * (n_x - 1)], S_GI + 1)
    either(left, mine, item_own.at[:, 0:sub * (n_e - 1)], item_own, S_OWN)

    either(arrived, fin_mine, fin_all.at[0:n_b - 1], fin_all, S_FIN)
    n_t = n_x * n_c
    here = chip * n_c + lax.div(core * n_c + col, 2)
    wide = jnp.concatenate([fin_all[here], fin_all[n_t + here]], axis=0).astype(F32)
    wide = jnp.where(lax.rem(col, 2) == 1, pltpu.roll(wide, lanes // 2, 1), wide)
    out_user[...] = wide[:, :lanes // 2].astype(BF16)
    by_tile = jnp.concatenate(
        [fin_all[s * n_t + t].astype(F32) for t in range(n_t) for s in range(2)], axis=0).astype(BF16)
    ids = trip[0:1, aligned(block * 128, 128, 128)]
    e_user = pick(one_hot(ids, 128), lax.div(ids, 128), by_tile, n_t)

    arrived(recv_d.at[0:n_b - 1], S_D)
    diff = recv_d[0]
    for i in range(1, n_b):
        diff = diff + recv_d[i]
    zpart[emb] = jnp.sum(e_user * diff, axis=0, keepdims=True)
    for (e_o,) in others(n_e):
        remote(zpart.at[emb], zpart.at[emb], S_Z, e_at[e_o], col, row).start()
    either(left, fin_mine, fin_all.at[0:n_b - 1], fin_all, S_FIN)
    left(recv_d.at[0:n_b - 1], S_D)
    arrived(zpart.at[0:n_e - 1], S_Z)
    score = zpart[0]
    for i in range(1, n_e):
        score = score + zpart[i]
    scores[block] = score
    for x_o, c_o, k_o in others(n_x, n_c, 2):
        remote(scores.at[block], scores.at[block], S_S, emb, c_at[c_o], x_at[x_o] * 2 + k_at[k_o]).start()
    left(zpart.at[0:n_e - 1], S_Z)
    arrived(scores.at[0:n_b - 1], S_S)
    for i in range(n_b):
        score_out[i:i + 1, :] = scores[i]
    left(scores.at[0:n_b - 1], S_S)


def finish(user_in, item_in, score_in, out_user, out_item, loss):
    out_user[...] = user_in[...]
    out_item[...] = item_in[...]
    loss[...] = jax.nn.softplus(-score_in[...])


def solution(mesh):
    dims = n_e, n_c, n_r = mesh.shape["emb"], mesh.shape["col"], mesh.shape["row"]

    def local_fn(mask_blk, user_sh, item_sh, triples):
        rows_u = mask_blk.shape[0]
        width, cols = item_sh.shape
        num_trip = triples.shape[0]
        n_x, n_p, n_b, half = n_r // 2, n_c * n_e, n_r * n_c, n_e // 2
        sub = width // n_e
        ni, cu, kd = n_r * sub, 2 * rows_u, half * cols
        piece, lanes = ni // n_x, cu // n_c
        dma = pltpu.SemaphoreType.DMA
        vmem, hbm = pl.BlockSpec(memory_space=pltpu.VMEM), pl.BlockSpec(memory_space=pltpu.HBM)
        scratch = [
            pltpu.VMEM((cols, user_sh.shape[0]), BF16),
            pltpu.VMEM((8, lanes), BF16),
            pltpu.VMEM((cols, lanes), F32),
            pltpu.VMEM((cols, width), BF16),
            pltpu.VMEM((3, num_trip), I32),
            pltpu.VMEM((n_r, rows_u, sub), I32),
            pltpu.VMEM((n_r, rows_u, width), I32),
            pltpu.VMEM((rows_u, 128), I32),
            pltpu.VMEM((cu, ni), BF16),
            pltpu.VMEM((cu, ni), BF16),
            pltpu.VMEM((n_r, 1, ni), I32),
            pltpu.VMEM((2 * n_c, 1, rows_u), I32),
            pltpu.VMEM((cu, 128), F32),
            pltpu.VMEM((2 * n_c * half, 8, lanes), BF16),
            pltpu.VMEM((kd, cu), F32),
            pltpu.VMEM((kd, ni), BF16),
            pltpu.VMEM((kd, ni), BF16),
            pltpu.VMEM((kd, ni), BF16),
            pltpu.VMEM((n_p, 8, lanes), BF16),
            pltpu.VMEM((n_p, 8, lanes), BF16),
            pltpu.VMEM((3, kd, cu), F32),
            pltpu.VMEM((3, n_p, 8, lanes), F32),
            pltpu.VMEM((3, kd, ni), F32),
            pltpu.VMEM((3, n_x, kd, piece), F32),
            pltpu.VMEM((1, 8, lanes), BF16),
            pltpu.VMEM((kd, piece), BF16),
            pltpu.VMEM((cols, width), BF16),
            pltpu.VMEM((2 * n_x * n_c, 8, lanes), BF16),
            pltpu.VMEM((2, LOW, num_trip), BF16),
            pltpu.VMEM((cols, num_trip), F32),
            pltpu.VMEM((n_b, cols, 128), F32),
            pltpu.VMEM((n_e, 1, 128), F32),
            pltpu.VMEM((n_b, 1, 128), F32),
            dma((n_r,)), dma((n_r,)), dma((3,)), dma((NUM_SEMS,)), dma((NUM_SEMS,)),
        ]
        user_t, item_t, score = pl.pallas_call(
            functools.partial(kernel, dims),
            out_shape=(jax.ShapeDtypeStruct((cols, user_sh.shape[0]), BF16),
                       jax.ShapeDtypeStruct((cols, width), BF16),
                       jax.ShapeDtypeStruct((n_b, 128), F32)),
            in_specs=[hbm, hbm, hbm, hbm],
            out_specs=(vmem, vmem, vmem),
            scratch_shapes=scratch,
            compiler_params=pltpu.CompilerParams(collective_id=0, has_side_effects=True, vmem_limit_bytes=40 << 20),
        )(mask_blk, *(pltpu.with_memory_space_constraint(v.T, pltpu.HBM) for v in (user_sh, item_sh, triples)))
        user_t, item_t, loss = pl.pallas_call(
            finish,
            out_shape=(jax.ShapeDtypeStruct(user_t.shape, BF16), jax.ShapeDtypeStruct(item_t.shape, BF16),
                       jax.ShapeDtypeStruct(score.shape, F32)),
            in_specs=[vmem] * 3,
            compiler_params=pltpu.CompilerParams(vmem_limit_bytes=1 << 20),
        )(user_t, item_t, score)
        return user_t.T, item_t.T, loss.reshape(num_trip)

    return jax.shard_map(
        local_fn, mesh=mesh,
        in_specs=(P("row", "col"), P(("row", "col"), "emb"), P(("col", "row"), "emb"), P()),
        out_specs=(P(("row", "col"), "emb"), P(("col", "row"), "emb"), P()),
        check_vma=False)
```

```python
import functools

import jax
import jax.numpy as jnp
from jax import lax
from jax.experimental import pallas as pl
from jax.experimental.pallas import tpu as pltpu
from jax.sharding import PartitionSpec as P

MESH = pl.DeviceIdType.MESH
F32, BF16, I32 = jnp.float32, jnp.bfloat16, jnp.int32
NUM_LAYERS = 3
CHUNK = 512
PICK = 1024
LOW = 256


def each(lo, hi, body):
    def step(i, carry):
        body(i)
        return carry

    lax.fori_loop(lo, hi, step, 0)


def aligned(start, size, unit):
    return pl.ds(pl.multiple_of(start, unit), size)


def lane_dot(lhs, rhs):
    return lax.dot_general(lhs, rhs, (((1,), (1,)), ((), ())), preferred_element_type=F32)


def far_first(*sizes):
    offsets = [()]
    for n in sizes:
        offsets = [(*o, i) for o in offsets for i in range(n)]
    return sorted(offsets, key=lambda o: -sum(min(i, n - i) for i, n in zip(o, sizes)))


def others(*sizes):
    offsets = [()]
    for n in sizes:
        offsets = [(*o, i) for o in offsets for i in range(n)]
    return offsets[1:]


(S_ITEM0, S_USER0, S_DI, S_DU, S_RU, S_RI, S_GU, S_GI, S_OWN, S_FIN, S_D, S_Z, S_S, S_SWAP, NUM_SEMS) = (
    0, 1, 2, 3, 4, 7, 10, 12, 14, 15, 16, 17, 18, 19, 20)


def kernel(dims, mask_hbm, user_hbm, item_hbm, trip_hbm, out_user, out_item, score_out,
           user_in, user_pack, user_wide, item_in, trip, mask_part, mask_raw, row_acc, mask_bf, adj, deg_item, deg_user, user_scale,
           user0_in, user0, item0, item1, item2,
           user1, user2, part_u, recv_u, part_i, recv_i,
           fin_tile, fin_item, item_own, fin_all, hot_item, part_d, recv_d, zpart, scores,
           sem_part, sem_raw, sem_in, sem_send, sem_recv):
    n_e, n_c, n_r = dims
    n_x, half = n_r // 2, n_e // 2
    n_p = n_c * n_e
    n_b = n_r * n_c
    emb, col, row = lax.axis_index("emb"), lax.axis_index("col"), lax.axis_index("row")
    chip, core = lax.div(row, 2), lax.rem(row, 2)
    rows_u = mask_hbm.shape[0]
    width = item_in.shape[1]
    sub = width // n_e
    cols = item_in.shape[0]
    kd, cu = part_u.shape[1:]
    ni = adj.shape[1]
    piece = ni // n_x
    lanes = cu // n_c
    plane = col * n_e + emb
    block = row * n_c + col
    home = lax.div(emb, half)
    in_half = lax.rem(emb, half)
    mine = home == core
    e_at = [lax.rem(emb + i, n_e) for i in range(n_e)]
    c_at = [lax.rem(col + i, n_c) for i in range(n_c)]
    x_at = [lax.rem(chip + i, n_x) for i in range(n_x)]
    k_at = [core, 1 - core]

    def remote(src, dst, stage, e, c, r):
        return pltpu.make_async_remote_copy(
            src_ref=src, dst_ref=dst, send_sem=sem_send.at[stage], recv_sem=sem_recv.at[stage],
            device_id=(e, c, r), device_id_type=MESH)

    def arrived(view, stage):
        remote(view, view, stage, emb, col, row).wait_recv()

    def left(view, stage):
        remote(view, view, stage, emb, col, row).wait_send()

    def either(wait, alone, less, full, stage):
        @pl.when(alone)
        def _():
            wait(less, stage)

        @pl.when(jnp.logical_not(alone))
        def _():
            wait(full, stage)

    def part(i):
        return pltpu.make_async_copy(
            mask_hbm.at[:, aligned(i * width + emb * sub, sub, 128)], mask_part.at[i], sem_part.at[i])

    def raw(i):
        return pltpu.make_async_copy(
            mask_hbm.at[:, i * width:(i + 1) * width], mask_raw.at[i], sem_raw.at[i])

    fetch = [pltpu.make_async_copy(src, dst, sem_in.at[i]) for i, (src, dst) in enumerate(
        ((user_hbm, user_in), (item_hbm, item_in), (trip_hbm, trip)))]

    for copy in fetch:
        copy.start()
    for i in range(n_r):
        part(i).start()

    barrier = pltpu.get_barrier_semaphore()

    def hello(e, c, r):
        pl.semaphore_signal(barrier, inc=1, device_id=(e, c, r), device_id_type=MESH)

    for x_o, e_o, k_o in far_first(n_x, n_e, 2)[:-1]:
        hello(e_at[e_o], col, x_at[x_o] * 2 + k_at[k_o])
    for c_o, e_o, k_o in far_first(n_c, n_e, 2):
        if c_o:
            hello(e_at[e_o], c_at[c_o], chip * 2 + k_at[k_o])

    own_users = aligned(core * rows_u, rows_u, 128)
    for i in range(n_r):
        part(i).wait()
    for i in range(n_r):
        raw(i).start()

    fetch[0].wait()
    user_wide[...] = jnp.zeros_like(user_wide)
    user_wide[:, 0:lanes // 2] = user_in[...].astype(F32)
    wide = user_wide[...]
    user_pack[...] = (wide[0:8] + pltpu.roll(wide[8:16], lanes // 2, 1)).astype(BF16)
    fetch[1].wait()
    fetch[2].wait()
    pl.semaphore_wait(barrier, n_r * n_e - 1 + 2 * n_e * (n_c - 1))

    here_rows = aligned(in_half * cols, cols, 16)
    here_items = aligned(row * sub, sub, 128)
    user_slot = (core * n_c + col) * half + in_half

    def user0_send(c_o, e_o):
        remote(user_pack, user0_in.at[user_slot], S_USER0, e_at[e_o], c_at[c_o], chip * 2 + home).start()

    for c_o, e_o in others(n_c, n_e):
        user0_send(c_o, e_o)
    def item0_send(x_o, e_o):
        remote(item_in.at[:, aligned(e_at[e_o] * sub, sub, 128)], item0.at[here_rows, here_items], S_ITEM0,
               e_at[e_o], col, x_at[x_o] * 2 + home).start()

    for x_o, e_o in others(n_x, n_e):
        item0_send(x_o, e_o)

    @pl.when(jnp.logical_not(mine))
    def _():
        user0_send(0, 0)
        item0_send(0, 0)

    @pl.when(mine)
    def _():
        item0[here_rows, here_items] = item_in[:, aligned(emb * sub, sub, 128)]
        user0_in[user_slot] = user_pack[...]

    for i in range(n_r):
        mask_bf[own_users, i * sub:(i + 1) * sub] = mask_part[i].astype(F32).astype(BF16)
    deg_item[row] = jnp.dot(
        jnp.ones((8, rows_u), BF16), mask_bf[own_users, :], preferred_element_type=F32)[0:1].astype(I32)

    for x_o, k_o in others(n_x, 2):
        remote(deg_item.at[row], deg_item.at[row], S_DI, emb, col, x_at[x_o] * 2 + k_at[k_o]).start()

    remote(mask_bf.at[own_users], mask_bf.at[own_users], S_SWAP, emb, col, chip * 2 + 1 - core).start()

    for i in range(n_r):
        raw(i).wait()

        def row_sums(t):
            rs = aligned(t * 64, 64, 64)
            total = mask_raw[i, rs, 0:128]
            for j in range(1, width // 128):
                total = total + mask_raw[i, rs, j * 128:(j + 1) * 128]
            row_acc[rs, :] = total if i == 0 else row_acc[rs, :] + total

        each(0, rows_u // 64, row_sums)
    own_part = core * n_c + col
    deg_user[own_part] = jnp.sum(jnp.transpose(row_acc[...].astype(F32)), axis=0, keepdims=True).astype(I32)
    for c_o, k_o in others(n_c, 2):
        remote(deg_user.at[own_part], deg_user.at[own_part], S_DU, emb, c_at[c_o], chip * 2 + k_at[k_o]).start()

    def one_hot(ids, size):
        return (lax.broadcasted_iota(I32, (size, ids.shape[1]), 0) == lax.rem(ids, size)).astype(F32).astype(BF16)

    def hot_items(i):
        at = aligned(i * CHUNK, CHUNK, 128)
        for j in range(2):
            hot_item[j, :, at] = one_hot(trip[j + 1:j + 2, at], LOW)

    each(0, trip.shape[1] // CHUNK, hot_items)

    arrived(deg_item.at[0:n_r - 1], S_DI)
    arrived(deg_user.at[0:2 * n_c - 1], S_DU)
    total_i = deg_item[0]
    for i in range(1, n_r):
        total_i = total_i + deg_item[i]
    totals = []
    for k in range(2):
        total = deg_user[k * n_c]
        for i in range(1, n_c):
            total = total + deg_user[k * n_c + i]
        totals.append(total)
    total_u = jnp.concatenate(totals, axis=1)
    inv_item = lax.rsqrt(jnp.maximum(total_i, 1).astype(F32))
    inv_user = lax.rsqrt(jnp.maximum(total_u, 1).astype(F32))
    user_scale[...] = jnp.transpose(jnp.broadcast_to(inv_user, (128, cu)))

    def scale_rows(i):
        rs = aligned(i * 32, 32, 32)
        by_user = user_scale[rs, :]
        for j in range(ni // 128):
            js = slice(j * 128, (j + 1) * 128)
            adj[rs, js] = ((by_user * mask_bf[rs, js].astype(F32)) * inv_item[:, js]).astype(BF16)

    arrived(mask_bf.at[own_users], S_SWAP)
    each(0, cu // 32, scale_rows)

    own_items = aligned(chip * piece, piece, 128)
    own_rows, own_lanes = aligned(emb * 8, 8, 8), aligned(col * lanes, lanes, 128)

    def step_u(k, items):
        pairs = n_c // 2
        mate = lax.rem(col, 2)
        for (p_o,) in far_first(pairs):
            p_to = lax.rem(lax.div(col, 2) + p_o, pairs)
            both = aligned(p_to * 2 * lanes, 2 * lanes, 128)
            part_u[k, :, both] = lane_dot(items, adj[both, :])
            for c_o in (1, 0):
                c_to = p_to * 2 + lax.rem(mate + c_o, 2)
                for (e_o,) in far_first(n_e):
                    tile = part_u.at[k, aligned(e_at[e_o] * 8, 8, 8), aligned(c_to * lanes, lanes, 128)]
                    if p_o or c_o or e_o:
                        remote(tile, recv_u.at[k, plane], S_RU + k, e_at[e_o], c_to, row).start()
                    else:
                        recv_u[k, plane] = tile[...]

    def step_i(k, users):
        for (x_o,) in (*others(n_x), (0,)):
            there = aligned(x_at[x_o] * piece, piece, 128)
            part = jnp.dot(users, adj[:, there], preferred_element_type=F32)
            if x_o:
                part_i[k, :, there] = part
                remote(part_i.at[k, :, there], recv_i.at[k, chip], S_RI + k, emb, col, x_at[x_o] * 2 + core).start()
            else:
                recv_i[k, chip] = part

    def sum_u(k):
        arrived(recv_u.at[k, 0:n_p - 1], S_RU + k)
        total = recv_u[k, 0]
        for i in range(1, n_p):
            total = total + recv_u[k, i]
        return total.astype(BF16)

    def sum_i(k):
        arrived(recv_i.at[k, 0:n_x - 1], S_RI + k)
        total = recv_i[k, 0]
        for i in range(1, n_x):
            total = total + recv_i[k, i]
        return total.astype(BF16)

    def share_u(buf, k):
        for c_o, e_o in others(n_c, n_e):
            remote(buf.at[plane], buf.at[plane], S_GU + k, e_at[e_o], c_at[c_o], row).start()

    def share_i(buf, k):
        for (x_o,) in others(n_x):
            remote(buf.at[:, own_items], buf.at[:, own_items], S_GI + k, emb, col, x_at[x_o] * 2 + core).start()

    def whole_u(buf, k):
        arrived(buf.at[0:n_p - 1], S_GU + k)
        return jnp.concatenate(
            [jnp.concatenate([buf[c * n_e + e].astype(F32) for c in range(n_c)], axis=1) for e in range(n_e)],
            axis=0).astype(BF16)

    def whole_i(buf, k):
        arrived(buf.at[:, 0:piece * (n_x - 1)], S_GI + k)
        return buf[...]

    either(arrived, mine, user0_in.at[0:n_p - 1], user0_in, S_USER0)
    low = lax.broadcasted_iota(I32, (8, lanes), 1) < lanes // 2
    for t in range(n_c):
        for i in range(half):
            one = user0_in[2 * t * half + i].astype(F32)
            two = user0_in[(2 * t + 1) * half + i].astype(F32)
            ts = slice(t * lanes, (t + 1) * lanes)
            user0[i * cols:i * cols + 8, ts] = jnp.where(low, one, pltpu.roll(two, lanes // 2, 1))
            user0[i * cols + 8:i * cols + 16, ts] = jnp.where(low, pltpu.roll(one, lanes // 2, 1), two)
    step_i(0, user0[...].astype(BF16))
    n_in = n_r * half
    either(arrived, mine, recv_d.at[0:n_in - 1], recv_d.at[0:n_in], S_ITEM0)
    step_u(0, item0[...])

    got = sum_i(0)
    item1[:, own_items] = got
    share_i(item1, 0)
    item_acc = item0[:, own_items].astype(F32) + got.astype(F32)
    got = sum_u(0)
    user1[plane] = got
    share_u(user1, 0)
    user_acc = user0[own_rows, own_lanes] + got.astype(F32)

    step_u(1, whole_i(item1, 0))
    step_i(1, whole_u(user1, 0))
    got = sum_u(1)
    user2[plane] = got
    share_u(user2, 1)
    user_acc = user_acc + got.astype(F32)
    got = sum_i(1)
    item2[:, own_items] = got
    share_i(item2, 1)
    item_acc = item_acc + got.astype(F32)

    step_i(2, whole_u(user2, 1))
    step_u(2, whole_i(item2, 1))

    item_acc = item_acc + sum_i(2).astype(F32)
    fin_item[...] = (item_acc / (NUM_LAYERS + 1)).astype(BF16)
    back = aligned(emb * sub, sub, 128)

    def own_send(e_o, k_o):
        e_to = lax.rem(in_half + e_o, half)
        remote(fin_item.at[aligned(e_to * cols, cols, 16), aligned(k_at[k_o] * sub, sub, 128)], item_own.at[:, back],
               S_OWN, half * core + e_to, col, chip * 2 + k_at[k_o]).start()

    for e_o, k_o in others(half, 2):
        own_send(e_o, k_o)

    @pl.when(jnp.logical_not(mine))
    def _():
        own_send(0, 0)

    @pl.when(mine)
    def _():
        item_own[:, back] = fin_item[here_rows, aligned(core * sub, sub, 128)]

    user_acc = user_acc + sum_u(2).astype(F32)
    fin_tile[0] = (user_acc / (NUM_LAYERS + 1)).astype(BF16)
    e_fin = half * core + lax.div(emb, 2)
    slot = lax.rem(emb, 2) * (n_x * n_c) + chip * n_c + col
    fin_mine = e_fin == emb

    def fin_send(x_o, c_o, k_o):
        remote(fin_tile.at[0], fin_all.at[slot], S_FIN, e_fin, c_at[c_o], x_at[x_o] * 2 + k_at[k_o]).start()

    for offsets in others(n_x, n_c, 2):
        fin_send(*offsets)

    @pl.when(jnp.logical_not(fin_mine))
    def _():
        fin_send(0, 0, 0)

    @pl.when(fin_mine)
    def _():
        fin_all[slot] = fin_tile[0]

    either(arrived, mine, item_own.at[:, 0:sub * (n_e - 1)], item_own, S_OWN)
    out_item[...] = item_own[...]

    n_hi = width // LOW
    by_hi = jnp.concatenate([item_own[:, j * LOW:(j + 1) * LOW] for j in range(n_hi)], axis=0)
    hi_base = (col * n_r + row) * n_hi

    def pick(hot, high, table, count):
        found = jnp.dot(table, hot, preferred_element_type=F32)
        total = jnp.zeros((cols, high.shape[1]), F32)
        for j in range(count):
            total = total + jnp.where(high == j, found[j * cols:(j + 1) * cols], 0.0)
        return total

    def pick_side(i, at):
        return pick(hot_item[i - 1, :, at], lax.div(trip[i:i + 1, at], LOW) - hi_base, by_hi, n_hi)

    n_chunk, per_chunk = trip.shape[1] // PICK, PICK // 128

    def d_send(q):
        @pl.when(q != block)
        def _():
            remote(part_d.at[:, aligned(q * 128, 128, 128)], recv_d.at[block], S_D,
                   emb, lax.rem(q, n_c), lax.div(q, n_c)).start()

    def pick_items(i):
        chunk = lax.rem(lax.div(block, per_chunk) + i, n_chunk)
        at = aligned(chunk * PICK, PICK, 128)
        part_d[:, at] = pick_side(1, at) - pick_side(2, at)
        for j in range(per_chunk):
            d_send(chunk * per_chunk + j)

    for (i,) in far_first(n_chunk):
        pick_items(i)
    recv_d[block] = part_d[:, aligned(block * 128, 128, 128)]

    left(mask_bf.at[own_users], S_SWAP)
    either(left, mine, recv_d.at[0:n_in - 1], recv_d.at[0:n_in], S_ITEM0)
    either(left, mine, user0_in.at[0:n_p - 1], user0_in, S_USER0)
    left(deg_item.at[0:n_r - 1], S_DI)
    left(deg_user.at[0:2 * n_c - 1], S_DU)
    for k in range(3):
        left(recv_u.at[k, 0:n_p - 1], S_RU + k)
        left(recv_i.at[k, 0:n_x - 1], S_RI + k)
    left(user1.at[0:n_p - 1], S_GU)
    left(user2.at[0:n_p - 1], S_GU + 1)
    left(item1.at[:, 0:piece * (n_x - 1)], S_GI)
    left(item2.at[:, 0:piece * (n_x - 1)], S_GI + 1)
    either(left, mine, item_own.at[:, 0:sub * (n_e - 1)], item_own, S_OWN)

    either(arrived, fin_mine, fin_all.at[0:n_b - 1], fin_all, S_FIN)
    n_t = n_x * n_c
    here = chip * n_c + lax.div(core * n_c + col, 2)
    wide = jnp.concatenate([fin_all[here], fin_all[n_t + here]], axis=0).astype(F32)
    wide = jnp.where(lax.rem(col, 2) == 1, pltpu.roll(wide, lanes // 2, 1), wide)
    out_user[...] = wide[:, :lanes // 2].astype(BF16)
    by_tile = jnp.concatenate(
        [fin_all[s * n_t + t].astype(F32) for t in range(n_t) for s in range(2)], axis=0).astype(BF16)
    ids = trip[0:1, aligned(block * 128, 128, 128)]
    e_user = pick(one_hot(ids, 128), lax.div(ids, 128), by_tile, n_t)

    arrived(recv_d.at[0:n_b - 1], S_D)
    diff = recv_d[0]
    for i in range(1, n_b):
        diff = diff + recv_d[i]
    zpart[emb] = jnp.sum(e_user * diff, axis=0, keepdims=True)
    for (e_o,) in others(n_e):
        remote(zpart.at[emb], zpart.at[emb], S_Z, e_at[e_o], col, row).start()
    either(left, fin_mine, fin_all.at[0:n_b - 1], fin_all, S_FIN)
    left(recv_d.at[0:n_b - 1], S_D)
    arrived(zpart.at[0:n_e - 1], S_Z)
    score = zpart[0]
    for i in range(1, n_e):
        score = score + zpart[i]
    scores[block] = score
    for x_o, c_o, k_o in others(n_x, n_c, 2):
        remote(scores.at[block], scores.at[block], S_S, emb, c_at[c_o], x_at[x_o] * 2 + k_at[k_o]).start()
    left(zpart.at[0:n_e - 1], S_Z)
    arrived(scores.at[0:n_b - 1], S_S)
    for i in range(n_b):
        score_out[i:i + 1, :] = scores[i]
    left(scores.at[0:n_b - 1], S_S)


def finish(user_in, item_in, score_in, out_user, out_item, loss):
    out_user[...] = user_in[...]
    out_item[...] = item_in[...]
    loss[...] = jax.nn.softplus(-score_in[...])


def solution(mesh):
    dims = n_e, n_c, n_r = mesh.shape["emb"], mesh.shape["col"], mesh.shape["row"]

    def local_fn(mask_blk, user_sh, item_sh, triples):
        rows_u = mask_blk.shape[0]
        width, cols = item_sh.shape
        num_trip = triples.shape[0]
        n_x, n_p, n_b, half = n_r // 2, n_c * n_e, n_r * n_c, n_e // 2
        sub = width // n_e
        ni, cu, kd = n_r * sub, 2 * rows_u, half * cols
        piece, lanes = ni // n_x, cu // n_c
        dma = pltpu.SemaphoreType.DMA
        vmem, hbm = pl.BlockSpec(memory_space=pltpu.VMEM), pl.BlockSpec(memory_space=pltpu.HBM)
        scratch = [
            pltpu.VMEM((cols, user_sh.shape[0]), BF16),
            pltpu.VMEM((8, lanes), BF16),
            pltpu.VMEM((cols, lanes), F32),
            pltpu.VMEM((cols, width), BF16),
            pltpu.VMEM((3, num_trip), I32),
            pltpu.VMEM((n_r, rows_u, sub), I32),
            pltpu.VMEM((n_r, rows_u, width), I32),
            pltpu.VMEM((rows_u, 128), I32),
            pltpu.VMEM((cu, ni), BF16),
            pltpu.VMEM((cu, ni), BF16),
            pltpu.VMEM((n_r, 1, ni), I32),
            pltpu.VMEM((2 * n_c, 1, rows_u), I32),
            pltpu.VMEM((cu, 128), F32),
            pltpu.VMEM((2 * n_c * half, 8, lanes), BF16),
            pltpu.VMEM((kd, cu), F32),
            pltpu.VMEM((kd, ni), BF16),
            pltpu.VMEM((kd, ni), BF16),
            pltpu.VMEM((kd, ni), BF16),
            pltpu.VMEM((n_p, 8, lanes), BF16),
            pltpu.VMEM((n_p, 8, lanes), BF16),
            pltpu.VMEM((3, kd, cu), F32),
            pltpu.VMEM((3, n_p, 8, lanes), F32),
            pltpu.VMEM((3, kd, ni), F32),
            pltpu.VMEM((3, n_x, kd, piece), F32),
            pltpu.VMEM((1, 8, lanes), BF16),
            pltpu.VMEM((kd, piece), BF16),
            pltpu.VMEM((cols, width), BF16),
            pltpu.VMEM((2 * n_x * n_c, 8, lanes), BF16),
            pltpu.VMEM((2, LOW, num_trip), BF16),
            pltpu.VMEM((cols, num_trip), F32),
            pltpu.VMEM((n_b, cols, 128), F32),
            pltpu.VMEM((n_e, 1, 128), F32),
            pltpu.VMEM((n_b, 1, 128), F32),
            dma((n_r,)), dma((n_r,)), dma((3,)), dma((NUM_SEMS,)), dma((NUM_SEMS,)),
        ]
        user_t, item_t, score = pl.pallas_call(
            functools.partial(kernel, dims),
            out_shape=(jax.ShapeDtypeStruct((cols, user_sh.shape[0]), BF16),
                       jax.ShapeDtypeStruct((cols, width), BF16),
                       jax.ShapeDtypeStruct((n_b, 128), F32)),
            in_specs=[hbm, hbm, hbm, hbm],
            out_specs=(vmem, vmem, vmem),
            scratch_shapes=scratch,
            compiler_params=pltpu.CompilerParams(collective_id=0, has_side_effects=True, vmem_limit_bytes=40 << 20),
        )(mask_blk, *(pltpu.with_memory_space_constraint(v.T, pltpu.HBM) for v in (user_sh, item_sh, triples)))
        user_t, item_t, loss = pl.pallas_call(
            finish,
            out_shape=(jax.ShapeDtypeStruct(user_t.shape, BF16), jax.ShapeDtypeStruct(item_t.shape, BF16),
                       jax.ShapeDtypeStruct(score.shape, F32)),
            in_specs=[vmem] * 3,
            compiler_params=pltpu.CompilerParams(vmem_limit_bytes=1 << 20),
        )(user_t, item_t, score)
        return user_t.T, item_t.T, loss.reshape(num_trip)

    return jax.shard_map(
        local_fn, mesh=mesh,
        in_specs=(P("row", "col"), P(("row", "col"), "emb"), P(("col", "row"), "emb"), P()),
        out_specs=(P(("row", "col"), "emb"), P(("col", "row"), "emb"), P()),
        check_vma=False)
```
